32 devices in a mesh: gx: 2 (over x), gy: 4 (over y, core), gz: 4 (over z).
Axes of the slice: x: 2, y: 2, z: 4, core: 2. Of those that a mesh axis runs over, the one named last changes fastest.
Arguments:
- state: float32 [53, 8, 16, 512], P(None, 'gx', 'gy', 'gz'), may hold values from -8 to 8
- diffusivity: float32 [53], replicated, may hold values from 0.01 to 0.08
- rates: float32 [53, 53], replicated, may hold values from -1.75 to 1.75
- inverse: float32 [53, 53, 8, 16, 512], P(None, None, 'gx', 'gy', 'gz'), may hold values from -3 to 5
- boundary: int32 [3], replicated, may hold values from 0 to 1, as said below
Outputs:
- new_state: float32 [53, 8, 16, 512], P(None, 'gx', 'gy', 'gz')
The draws below stay inside these ranges and needn't reach their ends.
Inputs may be any that keep to these rules, and one draw needn't show every extreme that they name: `boundary`: 1 marks a dimension with periodic faces, 0 one with mirrored walls; at least one dimension has each kind.
All inputs are finite; a program needn't handle non-finite values.
Results may differ from the reference program's by a relative error of at most 0.00014.
Values sent between devices are 32-bit elements; how exact they have to be, the bound alone decides.
No kernel may reach another device: no remote copies, remote signals or barrier semaphores. Data moves between devices by JAX's collectives and lax.ppermute only.
A program may use at most 128 MiB of HBM per device.

```python
import math
import jax
import jax.numpy as jnp
from jax import lax

S = 53
NEWTON = 2
NX = 8
NY = 16
NZ = 512


def draw_state(key, part):
    position = jnp.arange(NX, dtype=jnp.float32) / max(NX - 1, 1)
    growth = (1.0 + 2.0 * position)[None, :, None, None]
    rough = jax.random.truncated_normal(key, -4.0, 4.0, (S, NX, NY, NZ), jnp.float32)
    return rough * growth * 0.6


def draw_inverse(key, part):
    key_noise, key_diag = jax.random.split(jax.random.fold_in(key, 7), 2)
    noise = jax.random.truncated_normal(key_noise, -4.0, 4.0, (S, S, NX, NY, NZ), jnp.float32) * (0.4 / math.sqrt(S))
    diagonal = jax.random.uniform(key_diag, (S, 1, NX, NY, NZ), jnp.float32, 0.7, 1.3)
    identity = jnp.eye(S, dtype=jnp.float32)[:, :, None, None, None]
    matrix = identity * diagonal + noise
    return matrix


def draw_boundary(key, part):
    key_extra, key_order = jax.random.split(jax.random.fold_in(key, 11))
    extra = jax.random.randint(key_extra, (1,), 0, 2, jnp.int32)
    kinds = jnp.concatenate([jnp.array([0, 1], jnp.int32), extra])
    return jax.random.permutation(key_order, kinds).astype(jnp.int32)


def centred(own_key, dims, width, limit, kind=jnp.bfloat16):
    return jnp.clip(width * jax.random.normal(own_key, dims, jnp.float32), -limit, limit).astype(kind)


def setup_inputs(seed: int = 0) -> dict:
    arg_keys = jax.random.split(jax.random.key(seed), 6)
    return {
        "state": draw_state(jax.random.fold_in(arg_keys[5], 71), 0),
        "diffusivity": jnp.clip(jnp.exp(jax.random.uniform(arg_keys[1], (S,), jnp.float32, math.log(0.01), math.log(0.08))), 0.01, 0.08),
        "rates": centred(arg_keys[2], (S, S), (S // 4) ** -0.5, 1.75, jnp.float32),
        "inverse": draw_inverse(jax.random.fold_in(arg_keys[5], 71), 0),
        "boundary": draw_boundary(jax.random.fold_in(arg_keys[5], 71), 0),
    }


implicit_gamma = 0.2928932188134524
explicit_delta = -0.7071067811865475
rel_tol = 0.1
abs_tol = 0.05
drift_speed = 0.2

def extend_dim(field, dim, periodic):
    widths = [(0, 0)] * 4
    widths[dim] = (2, 2)
    cyclic = jnp.pad(field, widths, mode='wrap')
    mirror = jnp.pad(field, widths, mode='symmetric')
    return jnp.where(periodic, cyclic, mirror)

def stencil_terms(extended, dim):
    length = extended.shape[dim] - 4
    parts = [lax.slice_in_dim(extended, k, k + length, axis=dim) for k in range(5)]
    second = (-parts[0] + 16.0 * parts[1] - 30.0 * parts[2] + 16.0 * parts[3] - parts[4]) / 12.0
    return (second, parts[1])

def transport(field, diffusivity, boundary):
    lap_x, below_x = stencil_terms(extend_dim(field, 1, boundary[0] == 1), 1)
    lap_y, unused_y = stencil_terms(extend_dim(field, 2, boundary[1] == 1), 2)
    lap_z, unused_z = stencil_terms(extend_dim(field, 3, boundary[2] == 1), 3)
    return diffusivity[:, None, None, None] * (lap_x + lap_y + lap_z) - drift_speed * (field - below_x)

def chemistry(field, rates):
    return jnp.einsum('sj,jxyz->sxyz', rates, jnp.tanh(field), precision=lax.Precision.HIGHEST)

def newton_solve(base, inverse, rates, weights):
    guess = base
    for sweep in range(NEWTON):
        residual = guess - base - implicit_gamma * chemistry(guess, rates)
        update = jnp.einsum('sjxyz,jxyz->sxyz', inverse, residual, precision=lax.Precision.HIGHEST)
        norm_value = jnp.sqrt(jnp.mean(jnp.square(update * weights)))
        guess = guess - update / jnp.maximum(norm_value, 1.0)
    return guess

def reference(state, diffusivity, rates, inverse, boundary):
    weights = 1.0 / (rel_tol * jnp.abs(state) + abs_tol)
    first_rate = transport(state, diffusivity, boundary)
    section = newton_solve(state + implicit_gamma * first_rate, inverse, rates, weights)
    second_rate = transport(section, diffusivity, boundary)
    base = state + explicit_delta * first_rate + (1.0 - explicit_delta) * second_rate
    base = base + (1.0 - implicit_gamma) * chemistry(section, rates)
    return newton_solve(base, inverse, rates, weights)
```

```python
import functools

import jax
import jax.numpy as jnp
from jax import lax
from jax.experimental import pallas as pl
from jax.experimental.pallas import tpu as pltpu
from jax.sharding import PartitionSpec as P

NEWTON = 2
AXES = ("gx", "gy", "gz")
SUB = 8

implicit_gamma = 0.2928932188134524
explicit_delta = -0.7071067811865475
rel_tol = 0.1
abs_tol = 0.05
drift_speed = 0.2

VMEM = pl.BlockSpec(memory_space=pltpu.VMEM)
SMEM = pl.BlockSpec(memory_space=pltpu.SMEM)
f32 = jnp.float32


def iota(dim, lanes):
    return lax.broadcasted_iota(jnp.int32, (SUB, lanes), dim)


def turn(value, shift, axis):
    size = value.shape[axis]
    return pltpu.roll(value, shift % size, axis)


def groups_of(rows):
    return rows // SUB


def pack_faces(load, species, groups, lanes, tail_y, head_y, tail_z, head_z):
    row = iota(0, lanes) % 4
    lane = iota(1, lanes)
    per = lanes // 2
    packs = tail_z.shape[0] // SUB
    tails = [jnp.zeros((SUB, lanes), f32) for _ in range(packs)]
    heads = [jnp.zeros((SUB, lanes), f32) for _ in range(packs)]
    for s in range(species):
        v = [load(s, g) for g in range(groups)]
        for k in range(groups // 2):
            a, b = v[2 * k], v[2 * k + 1]
            tail_y[s, k * SUB : (k + 1) * SUB, :] = jnp.where(row >= 2, a, turn(b, -2, 0))
            head_y[s, k * SUB : (k + 1) * SUB, :] = jnp.where(row < 2, a, turn(b, 2, 0))
        for g in range(groups):
            p, q = divmod(s * groups + g, per)
            here = lane // 2 == q
            tails[p] = jnp.where(here, turn(v[g], 2 * q + 2, 1), tails[p])
            heads[p] = jnp.where(here, turn(v[g], 2 * q, 1), heads[p])
    for p in range(packs):
        tail_z[p * SUB : (p + 1) * SUB, :] = tails[p]
        head_z[p * SUB : (p + 1) * SUB, :] = heads[p]


def wall_flags(kinds):
    out = []
    for i, axis in enumerate(AXES):
        walled = kinds[i] == 0
        here, last = lax.axis_index(axis), lax.axis_size(axis) - 1
        out.append((walled & (here == 0), walled & (here == last)))
    return out


def transport(load, store, species, groups, lanes, faces, diffusivity, kinds):
    load_low, load_high, tail_y, head_y, tail_z, head_z, edges = faces
    (wall_x0, wall_x1), (wall_y0, wall_y1), (wall_z0, wall_z1) = wall_flags(kinds)
    row = iota(0, lanes) % 4
    lane = iota(1, lanes)
    low_half = iota(0, lanes) < 4
    zero = jnp.zeros((SUB, lanes), f32)

    def along(pos, length, wall0, wall1):
        w0 = jnp.where(wall0, 1.0, 0.0).astype(f32)
        w1 = jnp.where(wall1, 1.0, 0.0).astype(f32)
        at = lambda k: pos == k
        centre = jnp.where(at(0), 16.0 * w0, jnp.where(at(length - 1), 16.0 * w1, 0.0)) - 30.0
        up1 = jnp.where(at(0), 0.0, 16.0) - jnp.where(at(1), w0, 0.0) - jnp.where(at(length - 1), w1, 0.0)
        dn1 = jnp.where(at(length - 1), 0.0, 16.0) - jnp.where(at(0), w0, 0.0) - jnp.where(at(length - 2), w1, 0.0)
        up2 = jnp.where(pos < 2, 0.0, -1.0)
        dn2 = jnp.where(pos >= length - 2, 0.0, -1.0)
        return centre, up1, dn1, up2, dn2, 1.0 - w0, 1.0 - w1

    cy, uy1, dy1, uy2, dy2, keep_y0, keep_y1 = along(row, 4, wall_y0, wall_y1)
    cz, uz1, dz1, uz2, dz2, keep_z0, keep_z1 = along(lane, lanes, wall_z0, wall_z1)
    centre = cy + cz - 30.0
    a01 = jnp.where(row < 2, -keep_y0, 0.0)
    a0 = jnp.where(row == 0, 16.0 * keep_y0, 0.0)
    b23 = jnp.where(row >= 2, -keep_y1, 0.0)
    b3 = jnp.where(row == 3, 16.0 * keep_y1, 0.0)
    edge = (lane < 2) | (lane >= lanes - 2)
    per = lanes // 2
    packs = tail_z.shape[0] // SUB
    even = lane % 2 == 0
    first = lane % 4 < 2
    for p in range(packs):
        span = slice(p * SUB, (p + 1) * SUB)
        low, high = tail_z[span, :], head_z[span, :]
        low = (jnp.where(even, 16.0 * turn(low, -1, 1), 0.0) - low) * keep_z0
        high = (jnp.where(even, 0.0, 16.0 * turn(high, 1, 1)) - high) * keep_z1
        high = turn(high, -2, 1)
        edges[0, span, :] = jnp.where(first, low, high)
        edges[1, span, :] = jnp.where(first, high, low)

    for s in range(species):
        v = [load(s, g) for g in range(groups)]
        half = [turn(u, 4, 0) for u in v]
        ghost_low = jnp.where(wall_x0, half[0], load_low(s))
        ghost_high = jnp.where(wall_x1, half[-1], load_high(s))
        chain = [ghost_low] + v + [ghost_high]
        halves = [turn(ghost_low, 4, 0)] + half + [turn(ghost_high, 4, 0)]
        scale = diffusivity[s] * (1.0 / 12.0)
        for g in range(groups):
            u = v[g]
            below = jnp.where(low_half, halves[g], halves[g + 1])
            above = jnp.where(low_half, halves[g + 1], halves[g + 2])
            total = centre * u + 16.0 * (below + above) - (chain[g] + chain[g + 2])
            total = total + uy1 * turn(u, 1, 0) + dy1 * turn(u, -1, 0)
            total = total + uy2 * turn(u, 2, 0) + dy2 * turn(u, -2, 0)
            span = slice(g // 2 * SUB, (g // 2 + 1) * SUB)
            t, h = tail_y[s, span, :], head_y[s, span, :]
            if g % 2 == 0:
                total = total + a01 * turn(t, -2, 0) + a0 * turn(t, -3, 0)
                total = total + b23 * turn(h, 2, 0) + b3 * turn(h, 3, 0)
            else:
                total = total + a01 * t + a0 * turn(t, -1, 0)
                total = total + b23 * h + b3 * turn(h, 1, 0)
            total = total + uz1 * turn(u, 1, 1) + dz1 * turn(u, -1, 1)
            total = total + uz2 * turn(u, 2, 1) + dz2 * turn(u, -2, 1)
            p, q = divmod(s * groups + g, per)
            ends = turn(edges[q % 2, p * SUB : (p + 1) * SUB, :], -2 * q, 1)
            total = total + jnp.where(edge, ends, zero)
            store(s, g, u, scale * total - drift_speed * (u - below))


def chemistry(acts, rates, out, rows, lanes):
    padded = rates.shape[0]
    cols = [acts[pl.ds(r, padded, stride=rows), :] for r in range(rows)]
    made = jnp.dot(
        rates[...], jnp.concatenate(cols, axis=1), precision=lax.Precision.HIGHEST, preferred_element_type=f32
    )
    for r in range(rows):
        out[pl.ds(r, padded, stride=rows), :] = made[:, r * lanes : (r + 1) * lanes]


def blank_tail(acts, species, rows, lanes):
    padded = acts.shape[0] // rows
    if padded > species:
        acts[species * rows :, :] = jnp.zeros(((padded - species) * rows, lanes), f32)


def matvec(inverse, residual, weights, update, partial, species, rows, lanes, block=4):
    def some(first, count, squares):
        acc = [None] * count
        for j in range(species):
            g = residual[j * rows : (j + 1) * rows, :]
            for i in range(count):
                term = inverse[first + i, j] * g
                acc[i] = term if acc[i] is None else acc[i] + term
        for i in range(count):
            update[first + i] = acc[i]
            scaled = acc[i] * weights[first + i]
            squares = squares + scaled * scaled
        return squares

    squares = jnp.zeros((rows, lanes), f32)
    whole = species // block
    squares = lax.fori_loop(0, whole, lambda k, c: some(k * block, block, c), squares)
    if species % block:
        squares = some(whole * block, species % block, squares)
    partial[...] = jnp.broadcast_to(jnp.sum(squares, axis=0, keepdims=True), partial.shape)


def damping(parts, entries):
    total = jnp.sum(parts[...], axis=(0, 1), keepdims=True)
    return 1.0 / jnp.maximum(jnp.sqrt(total * (1.0 / entries)), 1.0)


def pack_kernel(state, tail_y, head_y, tail_z, head_z):
    species, rows, lanes = state.shape
    load = lambda s, g: state[s, g * SUB : (g + 1) * SUB, :]
    pack_faces(load, species, groups_of(rows), lanes, tail_y, head_y, tail_z, head_z)


def face_loads(refs, lanes):
    if len(refs) == 1:
        block = refs[0]
        rows = block.shape[1]
        return (lambda s: block[s, rows - SUB :, :]), (lambda s: block[s, :SUB, :])
    low, high = refs
    return (lambda s: low[s]), (lambda s: high[s])


def first_kernel(x_faces, state, *refs):
    xs, refs = refs[:x_faces], refs[x_faces:]
    tail_y, head_y, tail_z, head_z, diffusivity, kinds, rates, inverse = refs[:8]
    rate0, base, weights, update, partial, acts, made, edges = refs[8:]
    species, rows, lanes = state.shape
    groups = groups_of(rows)
    low, high = face_loads(xs, lanes)

    def store(s, g, u, e):
        span = slice(g * SUB, (g + 1) * SUB)
        rate0[s, span, :] = e
        b = u + implicit_gamma * e
        base[s, span, :] = b
        acts[s * rows + g * SUB : s * rows + (g + 1) * SUB, :] = jnp.tanh(b)
        weights[s, span, :] = 1.0 / (rel_tol * jnp.abs(u) + abs_tol)

    load = lambda s, g: state[s, g * SUB : (g + 1) * SUB, :]
    blank_tail(acts, species, rows, lanes)
    transport(load, store, species, groups, lanes, (low, high, tail_y, head_y, tail_z, head_z, edges), diffusivity, kinds)
    chemistry(acts, rates, made, rows, lanes)
    made[...] = made[...] * -implicit_gamma
    matvec(inverse, made, weights, update, partial, species, rows, lanes)


def next_kernel(entries, parts, base, update, weights, rates, inverse, guess, second, partial, acts, made):
    species, rows, lanes = base.shape
    scale = damping(parts, entries)
    blank_tail(acts, species, rows, lanes)
    for s in range(species):
        z = base[s] - update[s] * scale
        guess[s] = z
        acts[s * rows : (s + 1) * rows, :] = jnp.tanh(z)
    chemistry(acts, rates, made, rows, lanes)
    for s in range(species):
        span = slice(s * rows, (s + 1) * rows)
        made[span, :] = (guess[s] - base[s]) - implicit_gamma * made[span, :]
    matvec(inverse, made, weights, second, partial, species, rows, lanes)


def section_kernel(entries, parts, guess, update, section, tail_y, head_y, tail_z, head_z):
    species, rows, lanes = guess.shape
    scale = damping(parts, entries)

    def load(s, g):
        span = slice(g * SUB, (g + 1) * SUB)
        z = guess[s, span, :] - update[s, span, :] * scale
        section[s, span, :] = z
        return z

    pack_faces(load, species, groups_of(rows), lanes, tail_y, head_y, tail_z, head_z)


def second_kernel(x_faces, section, *refs):
    xs, refs = refs[:x_faces], refs[x_faces:]
    tail_y, head_y, tail_z, head_z, diffusivity, kinds, rates, inverse, state, rate0, weights = refs[:11]
    base, update, partial, acts, made, edges = refs[11:]
    species, rows, lanes = state.shape
    groups = groups_of(rows)
    low, high = face_loads(xs, lanes)

    def store(s, g, u, e):
        span = slice(g * SUB, (g + 1) * SUB)
        mixed = state[s, span, :] + explicit_delta * rate0[s, span, :] + (1.0 - explicit_delta) * e
        base[s, span, :] = mixed
        acts[s * rows + g * SUB : s * rows + (g + 1) * SUB, :] = jnp.tanh(u)

    load = lambda s, g: section[s, g * SUB : (g + 1) * SUB, :]
    blank_tail(acts, species, rows, lanes)
    transport(load, store, species, groups, lanes, (low, high, tail_y, head_y, tail_z, head_z, edges), diffusivity, kinds)
    chemistry(acts, rates, made, rows, lanes)
    for s in range(species):
        span = slice(s * rows, (s + 1) * rows)
        b = base[s] + (1.0 - implicit_gamma) * made[span, :]
        base[s] = b
        acts[span, :] = jnp.tanh(b)
    chemistry(acts, rates, made, rows, lanes)
    made[...] = made[...] * -implicit_gamma
    matvec(inverse, made, weights, update, partial, species, rows, lanes)


def last_kernel(entries, parts, guess, update, out):
    scale = damping(parts, entries)
    for s in range(guess.shape[0]):
        out[s] = guess[s] - update[s] * scale


def shaped(*dims):
    return jax.ShapeDtypeStruct(dims, f32)


def call(kernel, outs, specs, args, scratch=(), cost=0, limit=8 << 20, name=None):
    return pl.pallas_call(
        kernel,
        out_shape=outs,
        in_specs=specs,
        out_specs=jax.tree.map(lambda _: VMEM, outs),
        scratch_shapes=scratch,
        compiler_params=pltpu.CompilerParams(vmem_limit_bytes=limit),
        cost_estimate=pl.CostEstimate(flops=cost, bytes_accessed=cost, transcendentals=0),
        name=name,
    )(*args)


def ring(axis, step):
    count = lax.axis_size(axis)
    return [(i, (i + step) % count) for i in range(count)]


def exchange(block, tail_y, head_y, tail_z, head_z):
    rows = block.shape[1]
    if lax.axis_size("gx") == 2 and rows == 2 * SUB:
        xs = [lax.ppermute(block, "gx", ring("gx", 1))]
    else:
        low = lax.ppermute(block[:, rows - SUB :, :], "gx", ring("gx", 1))
        xs = [low, lax.ppermute(block[:, :SUB, :], "gx", ring("gx", -1))]
    ys = [lax.ppermute(tail_y, "gy", ring("gy", 1)), lax.ppermute(head_y, "gy", ring("gy", -1))]
    zs = [lax.ppermute(tail_z, "gz", ring("gz", 1)), lax.ppermute(head_z, "gz", ring("gz", -1))]
    return xs, ys + zs


def body(state, diffusivity, rates, inverse, boundary):
    species, nx, ny, lanes = state.shape
    rows = nx * ny
    groups = groups_of(rows)
    assert ny * 2 == SUB and groups % 2 == 0 and lanes == 128
    devices = lax.axis_size("gx") * lax.axis_size("gy") * lax.axis_size("gz")
    entries = float(species * rows * lanes * devices)
    padded = -(-species // SUB) * SUB
    packs = -(-species * groups * 2 // lanes)
    block = shaped(species, rows, lanes)
    faces = [shaped(species, groups // 2 * SUB, lanes)] * 2 + [shaped(packs * SUB, lanes)] * 2
    partial = shaped(devices, lanes)
    flat = pltpu.VMEM((padded * rows, lanes), f32)
    edges = pltpu.VMEM((2, packs * SUB, lanes), f32)

    state = state.reshape(species, rows, lanes)
    inverse = inverse.reshape(species, species, rows, lanes)
    rates = jnp.pad(rates, ((0, padded - species),) * 2)

    def total(part):
        return lax.all_to_all(part, AXES, 0, 0)

    packed = call(pack_kernel, faces, [VMEM], (state,), cost=1 << 20, name="pack")
    xs, others = exchange(state, *packed)
    n = len(xs)
    rate0, base, weights, update, part = call(
        functools.partial(first_kernel, n),
        [block, block, block, block, partial],
        [VMEM] * (n + 5) + [SMEM, SMEM, VMEM, VMEM],
        (state, *xs, *others, diffusivity, boundary, rates, inverse),
        [flat, flat, edges],
        cost=8 << 20,
        name="first",
    )
    newton = functools.partial(next_kernel, entries)

    def iterate(part, base, update):
        return call(
            newton,
            [block, block, partial],
            [VMEM] * 6,
            (total(part), base, update, weights, rates, inverse),
            [flat, flat],
            cost=8 << 20,
            name="newton",
        )

    for _ in range(NEWTON - 1):
        base, update, part = iterate(part, base, update)
    section, *packed = call(
        functools.partial(section_kernel, entries),
        [block] + faces,
        [VMEM] * 3,
        (total(part), base, update),
        cost=1 << 20,
        name="section",
    )
    xs, others = exchange(section, *packed)
    base, update, part = call(
        functools.partial(second_kernel, n),
        [block, block, partial],
        [VMEM] * (n + 5) + [SMEM, SMEM] + [VMEM] * 5,
        (section, *xs, *others, diffusivity, boundary, rates, inverse, state, rate0, weights),
        [flat, flat, edges],
        cost=8 << 20,
        name="second",
    )
    for _ in range(NEWTON - 1):
        base, update, part = iterate(part, base, update)
    out = call(
        functools.partial(last_kernel, entries), block, [VMEM] * 3, (total(part), base, update), cost=1 << 19, name="last"
    )
    return out.reshape(species, nx, ny, lanes)


def solution(mesh):
    in_specs = (P(None, "gx", "gy", "gz"), P(), P(), P(None, None, "gx", "gy", "gz"), P())
    out_specs = P(None, "gx", "gy", "gz")
    return jax.shard_map(body, mesh=mesh, in_specs=in_specs, out_specs=out_specs, check_vma=False)
```

```python
import functools

import jax
import jax.numpy as jnp
from jax import lax
from jax.experimental import pallas as pl
from jax.experimental.pallas import tpu as pltpu
from jax.sharding import PartitionSpec as P

NEWTON = 2
AXES = ("gx", "gy", "gz")
SUB = 8

implicit_gamma = 0.2928932188134524
explicit_delta = -0.7071067811865475
rel_tol = 0.1
abs_tol = 0.05
drift_speed = 0.2

VMEM = pl.BlockSpec(memory_space=pltpu.VMEM)
SMEM = pl.BlockSpec(memory_space=pltpu.SMEM)
f32 = jnp.float32


def iota(dim, lanes):
    return lax.broadcasted_iota(jnp.int32, (SUB, lanes), dim)


def turn(value, shift, axis):
    size = value.shape[axis]
    return pltpu.roll(value, shift % size, axis)


def groups_of(rows):
    return rows // SUB


def pack_faces(load, species, groups, lanes, tail_y, head_y, tail_z, head_z):
    row = iota(0, lanes) % 4
    lane = iota(1, lanes)
    per = lanes // 2
    packs = tail_z.shape[0] // SUB
    tails = [jnp.zeros((SUB, lanes), f32) for _ in range(packs)]
    heads = [jnp.zeros((SUB, lanes), f32) for _ in range(packs)]
    for s in range(species):
        v = [load(s, g) for g in range(groups)]
        for k in range(groups // 2):
            a, b = v[2 * k], v[2 * k + 1]
            tail_y[s, k * SUB : (k + 1) * SUB, :] = jnp.where(row >= 2, a, turn(b, -2, 0))
            head_y[s, k * SUB : (k + 1) * SUB, :] = jnp.where(row < 2, a, turn(b, 2, 0))
        for g in range(groups):
            p, q = divmod(s * groups + g, per)
            here = lane // 2 == q
            tails[p] = jnp.where(here, turn(v[g], 2 * q + 2, 1), tails[p])
            heads[p] = jnp.where(here, turn(v[g], 2 * q, 1), heads[p])
    for p in range(packs):
        tail_z[p * SUB : (p + 1) * SUB, :] = tails[p]
        head_z[p * SUB : (p + 1) * SUB, :] = heads[p]


def wall_flags(kinds):
    out = []
    for i, axis in enumerate(AXES):
        walled = kinds[i] == 0
        here, last = lax.axis_index(axis), lax.axis_size(axis) - 1
        out.append((walled & (here == 0), walled & (here == last)))
    return out


def transport(load, store, species, groups, lanes, faces, diffusivity, kinds):
    load_low, load_high, tail_y, head_y, tail_z, head_z, edges = faces
    (wall_x0, wall_x1), (wall_y0, wall_y1), (wall_z0, wall_z1) = wall_flags(kinds)
    row = iota(0, lanes) % 4
    lane = iota(1, lanes)
    low_half = iota(0, lanes) < 4
    zero = jnp.zeros((SUB, lanes), f32)

    def along(pos, length, wall0, wall1):
        w0 = jnp.where(wall0, 1.0, 0.0).astype(f32)
        w1 = jnp.where(wall1, 1.0, 0.0).astype(f32)
        at = lambda k: pos == k
        centre = jnp.where(at(0), 16.0 * w0, jnp.where(at(length - 1), 16.0 * w1, 0.0)) - 30.0
        up1 = jnp.where(at(0), 0.0, 16.0) - jnp.where(at(1), w0, 0.0) - jnp.where(at(length - 1), w1, 0.0)
        dn1 = jnp.where(at(length - 1), 0.0, 16.0) - jnp.where(at(0), w0, 0.0) - jnp.where(at(length - 2), w1, 0.0)
        up2 = jnp.where(pos < 2, 0.0, -1.0)
        dn2 = jnp.where(pos >= length - 2, 0.0, -1.0)
        return centre, up1, dn1, up2, dn2, 1.0 - w0, 1.0 - w1

    cy, uy1, dy1, uy2, dy2, keep_y0, keep_y1 = along(row, 4, wall_y0, wall_y1)
    cz, uz1, dz1, uz2, dz2, keep_z0, keep_z1 = along(lane, lanes, wall_z0, wall_z1)
    centre = cy + cz - 30.0
    a01 = jnp.where(row < 2, -keep_y0, 0.0)
    a0 = jnp.where(row == 0, 16.0 * keep_y0, 0.0)
    b23 = jnp.where(row >= 2, -keep_y1, 0.0)
    b3 = jnp.where(row == 3, 16.0 * keep_y1, 0.0)
    edge = (lane < 2) | (lane >= lanes - 2)
    per = lanes // 2
    packs = tail_z.shape[0] // SUB
    even = lane % 2 == 0
    first = lane % 4 < 2
    for p in range(packs):
        span = slice(p * SUB, (p + 1) * SUB)
        low, high = tail_z[span, :], head_z[span, :]
        low = (jnp.where(even, 16.0 * turn(low, -1, 1), 0.0) - low) * keep_z0
        high = (jnp.where(even, 0.0, 16.0 * turn(high, 1, 1)) - high) * keep_z1
        high = turn(high, -2, 1)
        edges[0, span, :] = jnp.where(first, low, high)
        edges[1, span, :] = jnp.where(first, high, low)

    for s in range(species):
        v = [load(s, g) for g in range(groups)]
        half = [turn(u, 4, 0) for u in v]
        ghost_low = jnp.where(wall_x0, half[0], load_low(s))
        ghost_high = jnp.where(wall_x1, half[-1], load_high(s))
        chain = [ghost_low] + v + [ghost_high]
        halves = [turn(ghost_low, 4, 0)] + half + [turn(ghost_high, 4, 0)]
        scale = diffusivity[s] * (1.0 / 12.0)
        for g in range(groups):
            u = v[g]
            below = jnp.where(low_half, halves[g], halves[g + 1])
            above = jnp.where(low_half, halves[g + 1], halves[g + 2])
            total = centre * u + 16.0 * (below + above) - (chain[g] + chain[g + 2])
            total = total + uy1 * turn(u, 1, 0) + dy1 * turn(u, -1, 0)
            total = total + uy2 * turn(u, 2, 0) + dy2 * turn(u, -2, 0)
            span = slice(g // 2 * SUB, (g // 2 + 1) * SUB)
            t, h = tail_y[s, span, :], head_y[s, span, :]
            if g % 2 == 0:
                total = total + a01 * turn(t, -2, 0) + a0 * turn(t, -3, 0)
                total = total + b23 * turn(h, 2, 0) + b3 * turn(h, 3, 0)
            else:
                total = total + a01 * t + a0 * turn(t, -1, 0)
                total = total + b23 * h + b3 * turn(h, 1, 0)
            total = total + uz1 * turn(u, 1, 1) + dz1 * turn(u, -1, 1)
            total = total + uz2 * turn(u, 2, 1) + dz2 * turn(u, -2, 1)
            p, q = divmod(s * groups + g, per)
            ends = turn(edges[q % 2, p * SUB : (p + 1) * SUB, :], -2 * q, 1)
            total = total + jnp.where(edge, ends, zero)
            store(s, g, u, scale * total - drift_speed * (u - below))


def spread_kernel(rates, upper, lower):
    species = rates.shape[0]
    size = species * SUB
    pick = lax.broadcasted_iota(jnp.int32, (size, species), 0) // SUB
    pick = jnp.where(pick == lax.broadcasted_iota(jnp.int32, (size, species), 1), 1.0, 0.0).astype(f32)
    wide = jnp.dot(pick, rates[...], precision=lax.Precision.HIGHEST, preferred_element_type=f32)
    wide = lax.dot_general(
        wide, pick, (((1,), (1,)), ((), ())), precision=lax.Precision.HIGHEST, preferred_element_type=f32
    )
    same = lax.broadcasted_iota(jnp.int32, (size, size), 0) % SUB
    same = same == lax.broadcasted_iota(jnp.int32, (size, size), 1) % SUB
    wide = jnp.where(same, wide, 0.0)
    high = wide.astype(jnp.bfloat16)
    upper[...] = high
    lower[...] = (wide - high.astype(f32)).astype(jnp.bfloat16)


def at(s, g, lanes):
    return slice(s * SUB, (s + 1) * SUB), slice(g * lanes, (g + 1) * lanes)


def chemistry(acts, upper, lower):
    values = acts[...]
    high = values.astype(jnp.bfloat16)
    low = (values - high.astype(f32)).astype(jnp.bfloat16)
    dot = functools.partial(jnp.dot, preferred_element_type=f32)
    return dot(upper[...], high) + (dot(upper[...], low) + dot(lower[...], high))


def matvec(inverse, residual, weights, update, partial, species, groups, lanes, block=8):
    def some(first, count, squares):
        out = []
        for h in range(groups):
            span = slice(h * SUB, (h + 1) * SUB)
            acc = [None] * count
            for j in range(species):
                g = residual[at(j, h, lanes)]
                for i in range(count):
                    term = inverse[first + i, j, span, :] * g
                    acc[i] = term if acc[i] is None else acc[i] + term
            total = squares[h]
            for i in range(count):
                update[first + i, span, :] = acc[i]
                scaled = acc[i] * weights[first + i, span, :]
                total = total + scaled * scaled
            out.append(total)
        return tuple(out)

    squares = (jnp.zeros((SUB, lanes), f32),) * groups
    whole = species // block
    squares = lax.fori_loop(0, whole, lambda k, c: some(k * block, block, c), squares)
    if species % block:
        squares = some(whole * block, species % block, squares)
    partial[...] = jnp.broadcast_to(jnp.sum(sum(squares), axis=0, keepdims=True), partial.shape)


def damping(parts, entries):
    total = jnp.sum(parts[...], axis=(0, 1), keepdims=True)
    return 1.0 / jnp.maximum(jnp.sqrt(total * (1.0 / entries)), 1.0)


def pack_kernel(state, tail_y, head_y, tail_z, head_z):
    species, rows, lanes = state.shape
    load = lambda s, g: state[s, g * SUB : (g + 1) * SUB, :]
    pack_faces(load, species, groups_of(rows), lanes, tail_y, head_y, tail_z, head_z)


def face_loads(refs, lanes):
    if len(refs) == 1:
        block = refs[0]
        rows = block.shape[1]
        return (lambda s: block[s, rows - SUB :, :]), (lambda s: block[s, :SUB, :])
    low, high = refs
    return (lambda s: low[s]), (lambda s: high[s])


def first_kernel(x_faces, state, *refs):
    xs, refs = refs[:x_faces], refs[x_faces:]
    tail_y, head_y, tail_z, head_z, diffusivity, kinds, upper, lower, inverse = refs[:9]
    rate0, base, weights, update, partial, acts, made, edges = refs[9:]
    species, rows, lanes = state.shape
    groups = groups_of(rows)
    low, high = face_loads(xs, lanes)

    def store(s, g, u, e):
        span = slice(g * SUB, (g + 1) * SUB)
        rate0[s, span, :] = e
        b = u + implicit_gamma * e
        base[s, span, :] = b
        acts[at(s, g, lanes)] = jnp.tanh(b)
        weights[s, span, :] = 1.0 / (rel_tol * jnp.abs(u) + abs_tol)

    load = lambda s, g: state[s, g * SUB : (g + 1) * SUB, :]
    transport(load, store, species, groups, lanes, (low, high, tail_y, head_y, tail_z, head_z, edges), diffusivity, kinds)
    made[...] = chemistry(acts, upper, lower) * -implicit_gamma
    matvec(inverse, made, weights, update, partial, species, groups, lanes)


def next_kernel(entries, parts, base, update, weights, upper, lower, inverse, guess, second, partial, acts, made):
    species, rows, lanes = base.shape
    groups = groups_of(rows)
    scale = damping(parts, entries)
    for s in range(species):
        for g in range(groups):
            span = slice(g * SUB, (g + 1) * SUB)
            z = base[s, span, :] - update[s, span, :] * scale
            guess[s, span, :] = z
            acts[at(s, g, lanes)] = jnp.tanh(z)
    made[...] = chemistry(acts, upper, lower)
    for s in range(species):
        for g in range(groups):
            span = slice(g * SUB, (g + 1) * SUB)
            gap = guess[s, span, :] - base[s, span, :]
            made[at(s, g, lanes)] = gap - implicit_gamma * made[at(s, g, lanes)]
    matvec(inverse, made, weights, second, partial, species, groups, lanes)


def section_kernel(entries, parts, guess, update, section, tail_y, head_y, tail_z, head_z):
    species, rows, lanes = guess.shape
    scale = damping(parts, entries)

    def load(s, g):
        span = slice(g * SUB, (g + 1) * SUB)
        z = guess[s, span, :] - update[s, span, :] * scale
        section[s, span, :] = z
        return z

    pack_faces(load, species, groups_of(rows), lanes, tail_y, head_y, tail_z, head_z)


def second_kernel(x_faces, section, *refs):
    xs, refs = refs[:x_faces], refs[x_faces:]
    tail_y, head_y, tail_z, head_z, diffusivity, kinds, upper, lower, inverse, state, rate0, weights = refs[:12]
    base, update, partial, acts, made, edges = refs[12:]
    species, rows, lanes = state.shape
    groups = groups_of(rows)
    low, high = face_loads(xs, lanes)

    def store(s, g, u, e):
        span = slice(g * SUB, (g + 1) * SUB)
        mixed = state[s, span, :] + explicit_delta * rate0[s, span, :] + (1.0 - explicit_delta) * e
        base[s, span, :] = mixed
        acts[at(s, g, lanes)] = jnp.tanh(u)

    load = lambda s, g: section[s, g * SUB : (g + 1) * SUB, :]
    transport(load, store, species, groups, lanes, (low, high, tail_y, head_y, tail_z, head_z, edges), diffusivity, kinds)
    made[...] = chemistry(acts, upper, lower)
    for s in range(species):
        for g in range(groups):
            span = slice(g * SUB, (g + 1) * SUB)
            b = base[s, span, :] + (1.0 - implicit_gamma) * made[at(s, g, lanes)]
            base[s, span, :] = b
            acts[at(s, g, lanes)] = jnp.tanh(b)
    made[...] = chemistry(acts, upper, lower) * -implicit_gamma
    matvec(inverse, made, weights, update, partial, species, groups, lanes)


def last_kernel(entries, parts, guess, update, out):
    scale = damping(parts, entries)
    for s in range(guess.shape[0]):
        out[s] = guess[s] - update[s] * scale


def shaped(*dims):
    return jax.ShapeDtypeStruct(dims, f32)


def call(kernel, outs, specs, args, scratch=(), cost=0, limit=8 << 20, name=None):
    return pl.pallas_call(
        kernel,
        out_shape=outs,
        in_specs=specs,
        out_specs=jax.tree.map(lambda _: VMEM, outs),
        scratch_shapes=scratch,
        compiler_params=pltpu.CompilerParams(vmem_limit_bytes=limit),
        cost_estimate=pl.CostEstimate(flops=cost, bytes_accessed=cost, transcendentals=0),
        name=name,
    )(*args)


def ring(axis, step):
    count = lax.axis_size(axis)
    return [(i, (i + step) % count) for i in range(count)]


def exchange(block, tail_y, head_y, tail_z, head_z):
    rows = block.shape[1]
    if lax.axis_size("gx") == 2 and rows == 2 * SUB:
        xs = [lax.ppermute(block, "gx", ring("gx", 1))]
    else:
        low = lax.ppermute(block[:, rows - SUB :, :], "gx", ring("gx", 1))
        xs = [low, lax.ppermute(block[:, :SUB, :], "gx", ring("gx", -1))]
    ys = [lax.ppermute(tail_y, "gy", ring("gy", 1)), lax.ppermute(head_y, "gy", ring("gy", -1))]
    zs = [lax.ppermute(tail_z, "gz", ring("gz", 1)), lax.ppermute(head_z, "gz", ring("gz", -1))]
    return xs, ys + zs


def body(state, diffusivity, rates, inverse, boundary):
    species, nx, ny, lanes = state.shape
    rows = nx * ny
    groups = groups_of(rows)
    assert ny * 2 == SUB and groups % 2 == 0 and lanes == 128
    devices = lax.axis_size("gx") * lax.axis_size("gy") * lax.axis_size("gz")
    entries = float(species * rows * lanes * devices)
    packs = -(-species * groups * 2 // lanes)
    block = shaped(species, rows, lanes)
    faces = [shaped(species, groups // 2 * SUB, lanes)] * 2 + [shaped(packs * SUB, lanes)] * 2
    partial = shaped(devices, lanes)
    flat = pltpu.VMEM((species * SUB, groups * lanes), f32)
    edges = pltpu.VMEM((2, packs * SUB, lanes), f32)

    state = state.reshape(species, rows, lanes)
    inverse = inverse.reshape(species, species, rows, lanes)
    half = jax.ShapeDtypeStruct((species * SUB,) * 2, jnp.bfloat16)
    rates = call(spread_kernel, [half, half], [VMEM], (rates,), cost=1 << 20, name="spread")

    def total(part):
        return lax.all_to_all(part, AXES, 0, 0)

    packed = call(pack_kernel, faces, [VMEM], (state,), cost=1 << 34, name="pack")
    xs, others = exchange(state, *packed)
    n = len(xs)
    rate0, base, weights, update, part = call(
        functools.partial(first_kernel, n),
        [block, block, block, block, partial],
        [VMEM] * (n + 5) + [SMEM, SMEM] + [VMEM] * 3,
        (state, *xs, *others, diffusivity, boundary, *rates, inverse),
        [flat, flat, edges],
        cost=8 << 20,
        name="first",
    )
    newton = functools.partial(next_kernel, entries)

    def iterate(part, base, update):
        return call(
            newton,
            [block, block, partial],
            [VMEM] * 7,
            (total(part), base, update, weights, *rates, inverse),
            [flat, flat],
            cost=8 << 20,
            name="newton",
        )

    for _ in range(NEWTON - 1):
        base, update, part = iterate(part, base, update)
    section, *packed = call(
        functools.partial(section_kernel, entries),
        [block] + faces,
        [VMEM] * 3,
        (total(part), base, update),
        cost=1 << 20,
        name="section",
    )
    xs, others = exchange(section, *packed)
    base, update, part = call(
        functools.partial(second_kernel, n),
        [block, block, partial],
        [VMEM] * (n + 5) + [SMEM, SMEM] + [VMEM] * 6,
        (section, *xs, *others, diffusivity, boundary, *rates, inverse, state, rate0, weights),
        [flat, flat, edges],
        cost=8 << 20,
        name="second",
    )
    for _ in range(NEWTON - 1):
        base, update, part = iterate(part, base, update)
    out = call(
        functools.partial(last_kernel, entries), block, [VMEM] * 3, (total(part), base, update), cost=1 << 19, name="last"
    )
    return out.reshape(species, nx, ny, lanes)


def solution(mesh):
    in_specs = (P(None, "gx", "gy", "gz"), P(), P(), P(None, None, "gx", "gy", "gz"), P())
    out_specs = P(None, "gx", "gy", "gz")
    return jax.shard_map(body, mesh=mesh, in_specs=in_specs, out_specs=out_specs, check_vma=False)
```

```python
import functools

import jax
import jax.numpy as jnp
from jax import lax
from jax.experimental import pallas as pl
from jax.experimental.pallas import tpu as pltpu
from jax.sharding import PartitionSpec as P

NEWTON = 2
AXES = ("gx", "gy", "gz")
SUB = 8

implicit_gamma = 0.2928932188134524
explicit_delta = -0.7071067811865475
rel_tol = 0.1
abs_tol = 0.05
drift_speed = 0.2

VMEM = pl.BlockSpec(memory_space=pltpu.VMEM)
SMEM = pl.BlockSpec(memory_space=pltpu.SMEM)
f32 = jnp.float32


def iota(dim, lanes):
    return lax.broadcasted_iota(jnp.int32, (SUB, lanes), dim)


def turn(value, shift, axis):
    size = value.shape[axis]
    return pltpu.roll(value, shift % size, axis)


def groups_of(rows):
    return rows // SUB


def pack_faces(load, species, groups, lanes, tail_y, head_y, tail_z, head_z):
    row = iota(0, lanes) % 4
    lane = iota(1, lanes)
    per = lanes // 2
    packs = tail_z.shape[0] // SUB
    tails = [jnp.zeros((SUB, lanes), f32) for _ in range(packs)]
    heads = [jnp.zeros((SUB, lanes), f32) for _ in range(packs)]
    for s in range(species):
        v = [load(s, g) for g in range(groups)]
        for k in range(groups // 2):
            a, b = v[2 * k], v[2 * k + 1]
            tail_y[s, k * SUB : (k + 1) * SUB, :] = jnp.where(row >= 2, a, turn(b, -2, 0))
            head_y[s, k * SUB : (k + 1) * SUB, :] = jnp.where(row < 2, a, turn(b, 2, 0))
        for g in range(groups):
            p, q = divmod(s * groups + g, per)
            here = lane // 2 == q
            tails[p] = jnp.where(here, turn(v[g], 2 * q + 2, 1), tails[p])
            heads[p] = jnp.where(here, turn(v[g], 2 * q, 1), heads[p])
    for p in range(packs):
        tail_z[p * SUB : (p + 1) * SUB, :] = tails[p]
        head_z[p * SUB : (p + 1) * SUB, :] = heads[p]


def wall_flags(kinds):
    out = []
    for i, axis in enumerate(AXES):
        walled = kinds[i] == 0
        here, last = lax.axis_index(axis), lax.axis_size(axis) - 1
        out.append((walled & (here == 0), walled & (here == last)))
    return out


def ghost_terms(low, high, scale, groups, sides):
    near_low, near_high = turn(low, 4, 0), turn(high, 4, 0)
    first = scale * (sides[2] * near_low - sides[0] * low) + sides[4] * near_low
    last = scale * (sides[3] * near_high - sides[1] * high)
    return [first] + [jnp.zeros_like(low)] * (groups - 2) + [last]


def prepare_ends(tail_z, head_z, sides, edges):
    lane = iota(1, tail_z.shape[1])
    even, first = lane % 2 == 0, lane % 4 < 2
    for p in range(tail_z.shape[0] // SUB):
        span = slice(p * SUB, (p + 1) * SUB)
        low, high = tail_z[span, :], head_z[span, :]
        low = (jnp.where(even, 16.0 * turn(low, -1, 1), 0.0) - low) * sides[5]
        high = (jnp.where(even, 0.0, 16.0 * turn(high, 1, 1)) - high) * sides[6]
        high = turn(high, -2, 1)
        edges[0, span, :] = jnp.where(first, low, high)
        edges[1, span, :] = jnp.where(first, high, low)


def row_terms(tail, head, k, sides):
    a01, a0, b23, b3 = sides[7:11]
    span = slice(k * SUB, (k + 1) * SUB)
    t, h = tail[span, :], head[span, :]
    first = a01 * turn(t, -2, 0) + a0 * turn(t, -3, 0) + b23 * turn(h, 2, 0) + b3 * turn(h, 3, 0)
    second = a01 * t + a0 * turn(t, -1, 0) + b23 * h + b3 * turn(h, 1, 0)
    return [first, second]


def end_terms(edges, rows, s, groups, scale):
    lanes = edges.shape[2]
    lane = iota(1, lanes)
    edge = (lane < 2) | (lane >= lanes - 2)
    out = []
    for g in range(groups):
        p, q = divmod(s * groups + g, lanes // 2)
        ends = turn(edges[q % 2, p * SUB : (p + 1) * SUB, :], -2 * q, 1)
        out.append(scale * (rows[g] + jnp.where(edge, ends, 0.0)))
    return out


def transport(load, store, species, groups, lanes, diffusivity, kinds):
    (wall_x0, wall_x1), (wall_y0, wall_y1), (wall_z0, wall_z1) = wall_flags(kinds)
    row = iota(0, lanes) % 4
    lane = iota(1, lanes)
    low_half = iota(0, lanes) < 4
    zero = jnp.zeros((SUB, lanes), f32)

    def along(pos, length, wall0, wall1):
        w0 = jnp.where(wall0, 1.0, 0.0).astype(f32)
        w1 = jnp.where(wall1, 1.0, 0.0).astype(f32)
        at = lambda k: pos == k
        centre = jnp.where(at(0), 16.0 * w0, jnp.where(at(length - 1), 16.0 * w1, 0.0)) - 30.0
        up1 = jnp.where(at(0), 0.0, 16.0) - jnp.where(at(1), w0, 0.0) - jnp.where(at(length - 1), w1, 0.0)
        dn1 = jnp.where(at(length - 1), 0.0, 16.0) - jnp.where(at(0), w0, 0.0) - jnp.where(at(length - 2), w1, 0.0)
        up2 = jnp.where(pos < 2, 0.0, -1.0)
        dn2 = jnp.where(pos >= length - 2, 0.0, -1.0)
        return centre, up1, dn1, up2, dn2

    cy, uy1, dy1, uy2, dy2 = along(row, 4, wall_y0, wall_y1)
    cz, uz1, dz1, uz2, dz2 = along(lane, lanes, wall_z0, wall_z1)
    centre = cy + cz - 30.0

    for s in range(species):
        v = [load(s, g) for g in range(groups)]
        half = [turn(u, 4, 0) for u in v]
        ghost_low = jnp.where(wall_x0, half[0], zero)
        ghost_high = jnp.where(wall_x1, half[-1], zero)
        chain = [ghost_low] + v + [ghost_high]
        halves = [turn(ghost_low, 4, 0)] + half + [turn(ghost_high, 4, 0)]
        scale = diffusivity[s] * (1.0 / 12.0)
        for g in range(groups):
            u = v[g]
            below = jnp.where(low_half, halves[g], halves[g + 1])
            above = jnp.where(low_half, halves[g + 1], halves[g + 2])
            total = centre * u + 16.0 * (below + above) - (chain[g] + chain[g + 2])
            total = total + uy1 * turn(u, 1, 0) + dy1 * turn(u, -1, 0)
            total = total + uy2 * turn(u, 2, 0) + dy2 * turn(u, -2, 0)
            total = total + uz1 * turn(u, 1, 1) + dz1 * turn(u, -1, 1)
            total = total + uz2 * turn(u, 2, 1) + dz2 * turn(u, -2, 1)
            store(s, g, u, scale * total - drift_speed * (u - below))


def stack_parts(parts, size):
    whole = size // 128 * 128
    return jnp.concatenate([p[:whole] for p in parts] + [p[whole:] for p in parts], axis=0)


def spread_kernel(rates, diffusivity, kinds, mix, scales, sides):
    species = rates.shape[0]
    size = species * SUB
    whole = size // 128 * 128
    part = size - whole

    def picks(rows, of):
        hit = of(lax.broadcasted_iota(jnp.int32, (rows, species), 0)) == lax.broadcasted_iota(jnp.int32, (rows, species), 1)
        return jnp.where(hit, 1.0, 0.0).astype(jnp.bfloat16)

    scaled = rates[...] * -implicit_gamma
    high = scaled.astype(jnp.bfloat16)
    low = (scaled - high.astype(f32)).astype(jnp.bfloat16)
    tall = picks(size, lambda i: i >> 3)

    def spread(piece, columns):
        rows = jnp.dot(tall, piece, preferred_element_type=f32).astype(jnp.bfloat16)
        full = lax.dot_general(rows, columns, (((1,), (1,)), ((), ())), preferred_element_type=f32)
        same = lax.broadcasted_iota(jnp.int32, full.shape, 0) & 7 == lax.broadcasted_iota(jnp.int32, full.shape, 1) & 7
        return jnp.where(same, full, 0.0)

    if whole:
        body = picks(whole, lambda i: i >> 3)
        front = spread(high, body).astype(jnp.bfloat16)
        mix[:, :whole] = front
        mix[:, whole : 2 * whole] = front
        mix[:, 2 * whole : 3 * whole] = spread(low, body).astype(jnp.bfloat16)
    if part:
        turns = lambda i: jnp.where(i < part, i, jnp.where(i < 2 * part, i - part, i - 2 * part))
        ends = picks(3 * part, lambda i: (turns(i) + whole) >> 3)
        column = lax.broadcasted_iota(jnp.int32, (size, 3 * part), 1)
        mix[:, 3 * whole :] = jnp.where(column < 2 * part, spread(high, ends), spread(low, ends)).astype(jnp.bfloat16)
    tile = scales.shape[1:]
    for s in range(species):
        scales[s] = jnp.full(tile, diffusivity[s] * (1.0 / 12.0), f32)
    keep = [jnp.where(w, 0.0, 1.0).astype(f32) for pair in wall_flags(kinds) for w in pair]
    keep0, keep1, y0, y1, keep2, keep3 = keep
    low_half = iota(0, tile[1]) < 4
    sides[0] = jnp.full(tile, keep0, f32)
    sides[1] = jnp.full(tile, keep1, f32)
    sides[2] = jnp.where(low_half, 16.0 * keep0, 0.0)
    sides[3] = jnp.where(low_half, 0.0, 16.0 * keep1)
    sides[4] = jnp.where(low_half, drift_speed * keep0, 0.0)
    sides[5] = jnp.full(tile, keep2, f32)
    sides[6] = jnp.full(tile, keep3, f32)
    row = iota(0, tile[1]) % 4
    sides[7] = jnp.where(row < 2, -y0, 0.0)
    sides[8] = jnp.where(row == 0, 16.0 * y0, 0.0)
    sides[9] = jnp.where(row >= 2, -y1, 0.0)
    sides[10] = jnp.where(row == 3, 16.0 * y1, 0.0)


def at(s, g, lanes):
    return slice(s * SUB, (s + 1) * SUB), slice(g * lanes, (g + 1) * lanes)


def chemistry(acts, mix):
    values = acts[...]
    high = values.astype(jnp.bfloat16).astype(f32)
    stack = stack_parts([high, values - high, high], values.shape[0]).astype(jnp.bfloat16)
    return jnp.dot(mix[...], stack, preferred_element_type=f32)


def matvec(inverse, residual, weights, update, partial, species, groups, lanes, block=8):
    def some(first, count, squares):
        out = []
        for h in range(groups):
            span = slice(h * SUB, (h + 1) * SUB)
            acc = [None] * count
            for j in range(species):
                g = residual[at(j, h, lanes)]
                for i in range(count):
                    term = inverse[first + i, j, span, :] * g
                    acc[i] = term if acc[i] is None else acc[i] + term
            total = squares[h]
            for i in range(count):
                update[first + i, span, :] = acc[i]
                scaled = acc[i] * weights[first + i, span, :]
                total = total + scaled * scaled
            out.append(total)
        return tuple(out)

    squares = (jnp.zeros((SUB, lanes), f32),) * groups
    whole = species // block
    squares = lax.fori_loop(0, whole, lambda k, c: some(k * block, block, c), squares)
    if species % block:
        squares = some(whole * block, species % block, squares)
    partial[...] = jnp.broadcast_to(jnp.sum(sum(squares), axis=0, keepdims=True), partial.shape)


def damping(parts, entries):
    total = jnp.sum(parts[...], axis=(0, 1), keepdims=True)
    return 1.0 / jnp.maximum(jnp.sqrt(total * (1.0 / entries)), 1.0)


def pack_kernel(state, tail_y, head_y, tail_z, head_z):
    species, rows, lanes = state.shape
    load = lambda s, g: state[s, g * SUB : (g + 1) * SUB, :]
    pack_faces(load, species, groups_of(rows), lanes, tail_y, head_y, tail_z, head_z)


def face_loads(refs, lanes):
    if len(refs) == 1:
        block = refs[0]
        rows = block.shape[1]
        return (lambda s: block[s, rows - SUB :, :]), (lambda s: block[s, :SUB, :])
    low, high = refs
    return (lambda s: low[s]), (lambda s: high[s])


def first_local_kernel(state, diffusivity, kinds, rate, weights):
    species, rows, lanes = state.shape
    groups = groups_of(rows)

    def store(s, g, u, e):
        span = slice(g * SUB, (g + 1) * SUB)
        rate[s, span, :] = e
        weights[s, span, :] = 1.0 / (rel_tol * jnp.abs(u) + abs_tol)

    load = lambda s, g: state[s, g * SUB : (g + 1) * SUB, :]
    transport(load, store, species, groups, lanes, diffusivity, kinds)


def first_kernel(x_faces, state, *refs):
    xs, refs = refs[:x_faces], refs[x_faces:]
    tail_y, head_y, tail_z, head_z, scales, sides, mix, inverse, rate, weights, rate0, base, update, partial, acts, made, edges = refs
    species, rows, lanes = state.shape
    groups = groups_of(rows)
    low, high = face_loads(xs, lanes)
    sides = [sides[i] for i in range(sides.shape[0])]
    prepare_ends(tail_z, head_z, sides, edges)
    for s in range(species):
        scale = scales[s]
        terms = ghost_terms(low(s), high(s), scale, groups, sides)
        rows_y = [t for k in range(groups // 2) for t in row_terms(tail_y[s], head_y[s], k, sides)]
        terms = [a + b for a, b in zip(terms, end_terms(edges, rows_y, s, groups, scale))]
        for g in range(groups):
            span = slice(g * SUB, (g + 1) * SUB)
            e = rate[s, span, :] + terms[g]
            rate0[s, span, :] = e
            b = state[s, span, :] + implicit_gamma * e
            base[s, span, :] = b
            acts[at(s, g, lanes)] = jnp.tanh(b)
    made[...] = chemistry(acts, mix)
    matvec(inverse, made, weights, update, partial, species, groups, lanes)


def next_kernel(entries, parts, base, update, weights, mix, inverse, guess, second, partial, acts, made):
    species, rows, lanes = base.shape
    groups = groups_of(rows)
    scale = damping(parts, entries)
    for s in range(species):
        for g in range(groups):
            span = slice(g * SUB, (g + 1) * SUB)
            z = base[s, span, :] - update[s, span, :] * scale
            guess[s, span, :] = z
            acts[at(s, g, lanes)] = jnp.tanh(z)
            made[at(s, g, lanes)] = z - base[s, span, :]
    made[...] = made[...] + chemistry(acts, mix)
    matvec(inverse, made, weights, second, partial, species, groups, lanes)


def second_local_kernel(
    section, diffusivity, kinds, mix, state, rate0, mixed, acts, made
):
    species, rows, lanes = state.shape
    groups = groups_of(rows)
    for s in range(species):
        for g in range(groups):
            acts[at(s, g, lanes)] = jnp.tanh(section[s, g * SUB : (g + 1) * SUB, :])
    made[...] = chemistry(acts, mix) * ((1.0 - implicit_gamma) / -implicit_gamma)

    def store(s, g, u, e):
        span = slice(g * SUB, (g + 1) * SUB)
        known = state[s, span, :] + explicit_delta * rate0[s, span, :] + (1.0 - explicit_delta) * e
        mixed[s, span, :] = known + made[at(s, g, lanes)]

    load = lambda s, g: section[s, g * SUB : (g + 1) * SUB, :]
    transport(load, store, species, groups, lanes, diffusivity, kinds)


def second_kernel(x_faces, mixed, *refs):
    xs, refs = refs[:x_faces], refs[x_faces:]
    tail_y, head_y, tail_z, head_z, scales, sides, mix, inverse, weights, base, update, partial, acts, made, edges = refs
    species, rows, lanes = mixed.shape
    groups = groups_of(rows)
    low, high = face_loads(xs, lanes)
    sides = [sides[i] for i in range(sides.shape[0])]
    prepare_ends(tail_z, head_z, sides, edges)
    for s in range(species):
        scale = scales[s]
        terms = ghost_terms(low(s), high(s), scale, groups, sides)
        rows_y = [t for k in range(groups // 2) for t in row_terms(tail_y[s], head_y[s], k, sides)]
        terms = [a + b for a, b in zip(terms, end_terms(edges, rows_y, s, groups, scale))]
        for g in range(groups):
            span = slice(g * SUB, (g + 1) * SUB)
            b = mixed[s, span, :] + (1.0 - explicit_delta) * terms[g]
            base[s, span, :] = b
            acts[at(s, g, lanes)] = jnp.tanh(b)
    made[...] = chemistry(acts, mix)
    matvec(inverse, made, weights, update, partial, species, groups, lanes)


def last_kernel(entries, parts, guess, update, out):
    scale = damping(parts, entries)
    for s in range(guess.shape[0]):
        out[s] = guess[s] - update[s] * scale


def shaped(*dims):
    return jax.ShapeDtypeStruct(dims, f32)


def call(kernel, outs, specs, args, scratch=(), cost=0, limit=8 << 20, name=None):
    return pl.pallas_call(
        kernel,
        out_shape=outs,
        in_specs=specs,
        out_specs=jax.tree.map(lambda _: VMEM, outs),
        scratch_shapes=scratch,
        compiler_params=pltpu.CompilerParams(vmem_limit_bytes=limit),
        cost_estimate=pl.CostEstimate(flops=cost, bytes_accessed=cost, transcendentals=0),
        name=name,
    )(*args)


def ring(axis, step):
    count = lax.axis_size(axis)
    return [(i, (i + step) % count) for i in range(count)]


def exchange(block, tail_y, head_y, tail_z, head_z):
    rows = block.shape[1]
    if lax.axis_size("gx") == 2 and rows == 2 * SUB:
        xs = [lax.ppermute(block, "gx", ring("gx", 1))]
    else:
        low = lax.ppermute(block[:, rows - SUB :, :], "gx", ring("gx", 1))
        xs = [low, lax.ppermute(block[:, :SUB, :], "gx", ring("gx", -1))]
    ys = [lax.ppermute(tail_y, "gy", ring("gy", 1)), lax.ppermute(head_y, "gy", ring("gy", -1))]
    zs = [lax.ppermute(tail_z, "gz", ring("gz", 1)), lax.ppermute(head_z, "gz", ring("gz", -1))]
    return xs, ys + zs


def body(state, diffusivity, rates, inverse, boundary):
    species, nx, ny, lanes = state.shape
    rows = nx * ny
    groups = groups_of(rows)
    assert ny * 2 == SUB and groups % 2 == 0 and lanes == 128
    devices = lax.axis_size("gx") * lax.axis_size("gy") * lax.axis_size("gz")
    entries = float(species * rows * lanes * devices)
    packs = -(-species * groups * 2 // lanes)
    block = shaped(species, rows, lanes)
    faces = [shaped(species, groups // 2 * SUB, lanes)] * 2 + [shaped(packs * SUB, lanes)] * 2
    partial = shaped(devices, lanes)
    flat = pltpu.VMEM((species * SUB, groups * lanes), f32)
    edges = pltpu.VMEM((2, packs * SUB, lanes), f32)

    state = state.reshape(species, rows, lanes)
    inverse = inverse.reshape(species, species, rows, lanes)
    mix, scales, sides = call(
        spread_kernel,
        [
            jax.ShapeDtypeStruct((species * SUB, 3 * species * SUB), jnp.bfloat16),
            shaped(species, SUB, lanes),
            shaped(11, SUB, lanes),
        ],
        [VMEM, SMEM, SMEM],
        (rates, diffusivity, boundary),
        cost=1 << 20,
        name="spread",
    )

    def total(part):
        return lax.all_to_all(part, AXES, 0, 0)

    packed = call(pack_kernel, faces, [VMEM], (state,), cost=1 << 34, name="pack")
    xs, others = exchange(state, *packed)
    n = len(xs)
    rate, weights = call(
        first_local_kernel,
        [block, block],
        [VMEM, SMEM, SMEM],
        (state, diffusivity, boundary),
        cost=1 << 23,
        name="first_local",
    )
    rate0, base, update, part = call(
        functools.partial(first_kernel, n),
        [block, block, block, partial],
        [VMEM] * (n + 11),
        (state, *xs, *others, scales, sides, mix, inverse, rate, weights),
        [flat, flat, edges],
        cost=1 << 23,
        name="first",
    )
    newton = functools.partial(next_kernel, entries)

    def iterate(part, base, update):
        return call(
            newton,
            [block, block, partial],
            [VMEM] * 6,
            (total(part), base, update, weights, mix, inverse),
            [flat, flat],
            cost=8 << 20,
            name="newton",
        )

    for _ in range(NEWTON - 1):
        base, update, part = iterate(part, base, update)
    section = call(
        functools.partial(last_kernel, entries), block, [VMEM] * 3, (total(part), base, update), cost=1 << 19, name="section"
    )
    packed = call(pack_kernel, faces, [VMEM], (section,), cost=1 << 20, name="pack_section")
    xs, others = exchange(section, *packed)
    mixed = call(
        second_local_kernel,
        block,
        [VMEM] + [SMEM, SMEM] + [VMEM] * 3,
        (section, diffusivity, boundary, mix, state, rate0),
        [flat, flat],
        cost=1 << 23,
        name="second_local",
    )
    base, update, part = call(
        functools.partial(second_kernel, n),
        [block, block, partial],
        [VMEM] * (n + 10),
        (mixed, *xs, *others, scales, sides, mix, inverse, weights),
        [flat, flat, edges],
        cost=1 << 23,
        name="second",
    )
    for _ in range(NEWTON - 1):
        base, update, part = iterate(part, base, update)
    out = call(
        functools.partial(last_kernel, entries), block, [VMEM] * 3, (total(part), base, update), cost=1 << 19, name="last"
    )
    return out.reshape(species, nx, ny, lanes)


def solution(mesh):
    in_specs = (P(None, "gx", "gy", "gz"), P(), P(), P(None, None, "gx", "gy", "gz"), P())
    out_specs = P(None, "gx", "gy", "gz")
    return jax.shard_map(body, mesh=mesh, in_specs=in_specs, out_specs=out_specs, check_vma=False)
```

```python
import functools

import jax
import jax.numpy as jnp
from jax import lax
from jax.experimental import pallas as pl
from jax.experimental.pallas import tpu as pltpu
from jax.sharding import PartitionSpec as P

NEWTON = 2
AXES = ("gx", "gy", "gz")
SUB = 8

implicit_gamma = 0.2928932188134524
explicit_delta = -0.7071067811865475
rel_tol = 0.1
abs_tol = 0.05
drift_speed = 0.2

VMEM = pl.BlockSpec(memory_space=pltpu.VMEM)
SMEM = pl.BlockSpec(memory_space=pltpu.SMEM)
f32 = jnp.float32


def iota(dim, lanes):
    return lax.broadcasted_iota(jnp.int32, (SUB, lanes), dim)


def turn(value, shift, axis):
    size = value.shape[axis]
    return pltpu.roll(value, shift % size, axis)


def groups_of(rows):
    return rows // SUB


def pack_faces(load, species, groups, lanes, tail_y, head_y, tail_z, head_z):
    row = iota(0, lanes) % 4
    lane = iota(1, lanes)
    per = lanes // 2
    packs = tail_z.shape[0] // SUB
    tails = [jnp.zeros((SUB, lanes), f32) for _ in range(packs)]
    heads = [jnp.zeros((SUB, lanes), f32) for _ in range(packs)]
    for s in range(species):
        v = [load(s, g) for g in range(groups)]
        for k in range(groups // 2):
            a, b = v[2 * k], v[2 * k + 1]
            tail_y[s, k * SUB : (k + 1) * SUB, :] = jnp.where(row >= 2, a, turn(b, -2, 0))
            head_y[s, k * SUB : (k + 1) * SUB, :] = jnp.where(row < 2, a, turn(b, 2, 0))
        for g in range(groups):
            p, q = divmod(s * groups + g, per)
            here = lane // 2 == q
            tails[p] = jnp.where(here, turn(v[g], 2 * q + 2, 1), tails[p])
            heads[p] = jnp.where(here, turn(v[g], 2 * q, 1), heads[p])
    for p in range(packs):
        tail_z[p * SUB : (p + 1) * SUB, :] = tails[p]
        head_z[p * SUB : (p + 1) * SUB, :] = heads[p]


def wall_flags(kinds):
    out = []
    for i, axis in enumerate(AXES):
        walled = kinds[i] == 0
        here, last = lax.axis_index(axis), lax.axis_size(axis) - 1
        out.append((walled & (here == 0), walled & (here == last)))
    return out


def ghost_terms(low, high, scale, groups, sides):
    near_low, near_high = turn(low, 4, 0), turn(high, 4, 0)
    first = scale * (sides[2] * near_low - sides[0] * low) + sides[4] * near_low
    last = scale * (sides[3] * near_high - sides[1] * high)
    return [first] + [jnp.zeros_like(low)] * (groups - 2) + [last]


def prepare_ends(tail_z, head_z, sides, edges):
    lane = iota(1, tail_z.shape[1])
    even, first = lane % 2 == 0, lane % 4 < 2
    for p in range(tail_z.shape[0] // SUB):
        span = slice(p * SUB, (p + 1) * SUB)
        low, high = tail_z[span, :], head_z[span, :]
        low = (jnp.where(even, 16.0 * turn(low, -1, 1), 0.0) - low) * sides[5]
        high = (jnp.where(even, 0.0, 16.0 * turn(high, 1, 1)) - high) * sides[6]
        high = turn(high, -2, 1)
        edges[0, span, :] = jnp.where(first, low, high)
        edges[1, span, :] = jnp.where(first, high, low)


def row_terms(tail, head, k, sides):
    a01, a0, b23, b3 = sides[7:11]
    span = slice(k * SUB, (k + 1) * SUB)
    t, h = tail[span, :], head[span, :]
    first = a01 * turn(t, -2, 0) + a0 * turn(t, -3, 0) + b23 * turn(h, 2, 0) + b3 * turn(h, 3, 0)
    second = a01 * t + a0 * turn(t, -1, 0) + b23 * h + b3 * turn(h, 1, 0)
    return [first, second]


def end_terms(edges, rows, s, groups, scale):
    lanes = edges.shape[2]
    lane = iota(1, lanes)
    edge = (lane < 2) | (lane >= lanes - 2)
    out = []
    for g in range(groups):
        p, q = divmod(s * groups + g, lanes // 2)
        ends = turn(edges[q % 2, p * SUB : (p + 1) * SUB, :], -2 * q, 1)
        out.append(scale * (rows[g] + jnp.where(edge, ends, 0.0)))
    return out


def transport(load, store, species, groups, lanes, diffusivity, kinds):
    (wall_x0, wall_x1), (wall_y0, wall_y1), (wall_z0, wall_z1) = wall_flags(kinds)
    row = iota(0, lanes) % 4
    lane = iota(1, lanes)
    low_half = iota(0, lanes) < 4
    zero = jnp.zeros((SUB, lanes), f32)

    def along(pos, length, wall0, wall1):
        w0 = jnp.where(wall0, 1.0, 0.0).astype(f32)
        w1 = jnp.where(wall1, 1.0, 0.0).astype(f32)
        at = lambda k: pos == k
        centre = jnp.where(at(0), 16.0 * w0, jnp.where(at(length - 1), 16.0 * w1, 0.0)) - 30.0
        up1 = jnp.where(at(0), 0.0, 16.0) - jnp.where(at(1), w0, 0.0) - jnp.where(at(length - 1), w1, 0.0)
        dn1 = jnp.where(at(length - 1), 0.0, 16.0) - jnp.where(at(0), w0, 0.0) - jnp.where(at(length - 2), w1, 0.0)
        up2 = jnp.where(pos < 2, 0.0, -1.0)
        dn2 = jnp.where(pos >= length - 2, 0.0, -1.0)
        return centre, up1, dn1, up2, dn2

    cy, uy1, dy1, uy2, dy2 = along(row, 4, wall_y0, wall_y1)
    cz, uz1, dz1, uz2, dz2 = along(lane, lanes, wall_z0, wall_z1)
    centre = cy + cz - 30.0

    for s in range(species):
        v = [load(s, g) for g in range(groups)]
        half = [turn(u, 4, 0) for u in v]
        ghost_low = jnp.where(wall_x0, half[0], zero)
        ghost_high = jnp.where(wall_x1, half[-1], zero)
        chain = [ghost_low] + v + [ghost_high]
        halves = [turn(ghost_low, 4, 0)] + half + [turn(ghost_high, 4, 0)]
        scale = diffusivity[s] * (1.0 / 12.0)
        for g in range(groups):
            u = v[g]
            below = jnp.where(low_half, halves[g], halves[g + 1])
            above = jnp.where(low_half, halves[g + 1], halves[g + 2])
            total = centre * u + 16.0 * (below + above) - (chain[g] + chain[g + 2])
            total = total + uy1 * turn(u, 1, 0) + dy1 * turn(u, -1, 0)
            total = total + uy2 * turn(u, 2, 0) + dy2 * turn(u, -2, 0)
            total = total + uz1 * turn(u, 1, 1) + dz1 * turn(u, -1, 1)
            total = total + uz2 * turn(u, 2, 1) + dz2 * turn(u, -2, 1)
            store(s, g, u, scale * total - drift_speed * (u - below))


def stack_parts(parts, size):
    whole = size // 128 * 128
    return jnp.concatenate([p[:whole] for p in parts] + [p[whole:] for p in parts], axis=0)


def spread_kernel(rates, diffusivity, kinds, mix, scales, sides):
    species = rates.shape[0]
    size = species * SUB
    whole = size // 128 * 128
    part = size - whole

    def picks(rows, of):
        hit = of(lax.broadcasted_iota(jnp.int32, (rows, species), 0)) == lax.broadcasted_iota(jnp.int32, (rows, species), 1)
        return jnp.where(hit, 1.0, 0.0).astype(jnp.bfloat16)

    scaled = rates[...] * -implicit_gamma
    high = scaled.astype(jnp.bfloat16)
    low = (scaled - high.astype(f32)).astype(jnp.bfloat16)
    tall = picks(size, lambda i: i >> 3)

    def spread(piece, columns):
        rows = jnp.dot(tall, piece, preferred_element_type=f32).astype(jnp.bfloat16)
        full = lax.dot_general(rows, columns, (((1,), (1,)), ((), ())), preferred_element_type=f32)
        same = lax.broadcasted_iota(jnp.int32, full.shape, 0) & 7 == lax.broadcasted_iota(jnp.int32, full.shape, 1) & 7
        return jnp.where(same, full, 0.0)

    if whole:
        body = picks(whole, lambda i: i >> 3)
        front = spread(high, body).astype(jnp.bfloat16)
        mix[:, :whole] = front
        mix[:, whole : 2 * whole] = front
        mix[:, 2 * whole : 3 * whole] = spread(low, body).astype(jnp.bfloat16)
    if part:
        turns = lambda i: jnp.where(i < part, i, jnp.where(i < 2 * part, i - part, i - 2 * part))
        ends = picks(3 * part, lambda i: (turns(i) + whole) >> 3)
        column = lax.broadcasted_iota(jnp.int32, (size, 3 * part), 1)
        mix[:, 3 * whole :] = jnp.where(column < 2 * part, spread(high, ends), spread(low, ends)).astype(jnp.bfloat16)
    tile = scales.shape[1:]
    for s in range(species):
        scales[s] = jnp.full(tile, diffusivity[s] * (1.0 / 12.0), f32)
    keep = [jnp.where(w, 0.0, 1.0).astype(f32) for pair in wall_flags(kinds) for w in pair]
    keep0, keep1, y0, y1, keep2, keep3 = keep
    low_half = iota(0, tile[1]) < 4
    sides[0] = jnp.full(tile, keep0, f32)
    sides[1] = jnp.full(tile, keep1, f32)
    sides[2] = jnp.where(low_half, 16.0 * keep0, 0.0)
    sides[3] = jnp.where(low_half, 0.0, 16.0 * keep1)
    sides[4] = jnp.where(low_half, drift_speed * keep0, 0.0)
    sides[5] = jnp.full(tile, keep2, f32)
    sides[6] = jnp.full(tile, keep3, f32)
    row = iota(0, tile[1]) % 4
    sides[7] = jnp.where(row < 2, -y0, 0.0)
    sides[8] = jnp.where(row == 0, 16.0 * y0, 0.0)
    sides[9] = jnp.where(row >= 2, -y1, 0.0)
    sides[10] = jnp.where(row == 3, 16.0 * y1, 0.0)


def at(s, g, lanes):
    return slice(s * SUB, (s + 1) * SUB), slice(g * lanes, (g + 1) * lanes)


def chemistry(acts, mix):
    values = acts[...]
    high = values.astype(jnp.bfloat16).astype(f32)
    stack = stack_parts([high, values - high, high], values.shape[0]).astype(jnp.bfloat16)
    return jnp.dot(mix[...], stack, preferred_element_type=f32)


def matvec(inverse, residual, weights, update, partial, species, groups, lanes, block=8):
    def some(first, count, squares):
        out = []
        for h in range(groups):
            span = slice(h * SUB, (h + 1) * SUB)
            acc = [None] * count
            for j in range(species):
                g = residual[at(j, h, lanes)]
                for i in range(count):
                    term = inverse[first + i, j, span, :] * g
                    acc[i] = term if acc[i] is None else acc[i] + term
            total = squares[h]
            for i in range(count):
                update[first + i, span, :] = acc[i]
                scaled = acc[i] * weights[first + i, span, :]
                total = total + scaled * scaled
            out.append(total)
        return tuple(out)

    squares = (jnp.zeros((SUB, lanes), f32),) * groups
    whole = species // block
    squares = lax.fori_loop(0, whole, lambda k, c: some(k * block, block, c), squares)
    if species % block:
        squares = some(whole * block, species % block, squares)
    partial[...] = jnp.broadcast_to(jnp.sum(sum(squares), axis=0, keepdims=True), partial.shape)


def damping(parts, entries):
    total = jnp.sum(parts[...], axis=(0, 1), keepdims=True)
    return 1.0 / jnp.maximum(jnp.sqrt(total * (1.0 / entries)), 1.0)


def pack_kernel(state, tail_y, head_y, tail_z, head_z):
    species, rows, lanes = state.shape
    load = lambda s, g: state[s, g * SUB : (g + 1) * SUB, :]
    pack_faces(load, species, groups_of(rows), lanes, tail_y, head_y, tail_z, head_z)


def face_loads(refs, lanes):
    if len(refs) == 1:
        block = refs[0]
        rows = block.shape[1]
        return (lambda s: block[s, rows - SUB :, :]), (lambda s: block[s, :SUB, :])
    low, high = refs
    return (lambda s: low[s]), (lambda s: high[s])


def first_local_kernel(state, diffusivity, kinds, rate, weights):
    species, rows, lanes = state.shape
    groups = groups_of(rows)

    def store(s, g, u, e):
        span = slice(g * SUB, (g + 1) * SUB)
        rate[s, span, :] = e
        weights[s, span, :] = 1.0 / (rel_tol * jnp.abs(u) + abs_tol)

    load = lambda s, g: state[s, g * SUB : (g + 1) * SUB, :]
    transport(load, store, species, groups, lanes, diffusivity, kinds)


def first_kernel(x_faces, state, *refs):
    xs, refs = refs[:x_faces], refs[x_faces:]
    tail_y, head_y, tail_z, head_z, scales, sides, mix, inverse, rate, weights, rate0, base, update, partial, acts, made, edges = refs
    species, rows, lanes = state.shape
    groups = groups_of(rows)
    low, high = face_loads(xs, lanes)
    sides = [sides[i] for i in range(sides.shape[0])]
    prepare_ends(tail_z, head_z, sides, edges)
    for s in range(species):
        scale = scales[s]
        terms = ghost_terms(low(s), high(s), scale, groups, sides)
        rows_y = [t for k in range(groups // 2) for t in row_terms(tail_y[s], head_y[s], k, sides)]
        terms = [a + b for a, b in zip(terms, end_terms(edges, rows_y, s, groups, scale))]
        for g in range(groups):
            span = slice(g * SUB, (g + 1) * SUB)
            e = rate[s, span, :] + terms[g]
            rate0[s, span, :] = e
            b = state[s, span, :] + implicit_gamma * e
            base[s, span, :] = b
            acts[at(s, g, lanes)] = jnp.tanh(b)
    made[...] = chemistry(acts, mix)
    matvec(inverse, made, weights, update, partial, species, groups, lanes)


def next_kernel(entries, parts, base, update, weights, mix, inverse, guess, second, partial, acts, made):
    species, rows, lanes = base.shape
    groups = groups_of(rows)
    scale = damping(parts, entries)
    for s in range(species):
        for g in range(groups):
            span = slice(g * SUB, (g + 1) * SUB)
            z = base[s, span, :] - update[s, span, :] * scale
            guess[s, span, :] = z
            acts[at(s, g, lanes)] = jnp.tanh(z)
            made[at(s, g, lanes)] = z - base[s, span, :]
    made[...] = made[...] + chemistry(acts, mix)
    matvec(inverse, made, weights, second, partial, species, groups, lanes)


def second_local_kernel(
    section, diffusivity, kinds, mix, state, rate0, mixed, acts, made
):
    species, rows, lanes = state.shape
    groups = groups_of(rows)
    for s in range(species):
        for g in range(groups):
            acts[at(s, g, lanes)] = jnp.tanh(section[s, g * SUB : (g + 1) * SUB, :])
    made[...] = chemistry(acts, mix) * ((1.0 - implicit_gamma) / -implicit_gamma)

    def store(s, g, u, e):
        span = slice(g * SUB, (g + 1) * SUB)
        known = state[s, span, :] + explicit_delta * rate0[s, span, :] + (1.0 - explicit_delta) * e
        mixed[s, span, :] = known + made[at(s, g, lanes)]

    load = lambda s, g: section[s, g * SUB : (g + 1) * SUB, :]
    transport(load, store, species, groups, lanes, diffusivity, kinds)


def second_kernel(x_faces, mixed, *refs):
    xs, refs = refs[:x_faces], refs[x_faces:]
    tail_y, head_y, tail_z, head_z, scales, sides, mix, inverse, weights, base, update, partial, acts, made, edges = refs
    species, rows, lanes = mixed.shape
    groups = groups_of(rows)
    low, high = face_loads(xs, lanes)
    sides = [sides[i] for i in range(sides.shape[0])]
    prepare_ends(tail_z, head_z, sides, edges)
    for s in range(species):
        scale = scales[s]
        terms = ghost_terms(low(s), high(s), scale, groups, sides)
        rows_y = [t for k in range(groups // 2) for t in row_terms(tail_y[s], head_y[s], k, sides)]
        terms = [a + b for a, b in zip(terms, end_terms(edges, rows_y, s, groups, scale))]
        for g in range(groups):
            span = slice(g * SUB, (g + 1) * SUB)
            b = mixed[s, span, :] + (1.0 - explicit_delta) * terms[g]
            base[s, span, :] = b
            acts[at(s, g, lanes)] = jnp.tanh(b)
    made[...] = chemistry(acts, mix)
    matvec(inverse, made, weights, update, partial, species, groups, lanes)


def last_kernel(entries, parts, guess, update, out):
    scale = damping(parts, entries)
    for s in range(guess.shape[0]):
        out[s] = guess[s] - update[s] * scale


def shaped(*dims):
    return jax.ShapeDtypeStruct(dims, f32)


def call(kernel, outs, specs, args, scratch=(), cost=0, limit=(6 << 20) + 1024, name=None):
    return pl.pallas_call(
        kernel,
        out_shape=outs,
        in_specs=specs,
        out_specs=jax.tree.map(lambda _: VMEM, outs),
        scratch_shapes=scratch,
        compiler_params=pltpu.CompilerParams(vmem_limit_bytes=limit),
        cost_estimate=pl.CostEstimate(flops=cost, bytes_accessed=cost, transcendentals=0),
        name=name,
    )(*args)


def ring(axis, step):
    count = lax.axis_size(axis)
    return [(i, (i + step) % count) for i in range(count)]


def exchange(block, tail_y, head_y, tail_z, head_z):
    rows = block.shape[1]
    if lax.axis_size("gx") == 2 and rows == 2 * SUB:
        xs = [lax.ppermute(block, "gx", ring("gx", 1))]
    else:
        low = lax.ppermute(block[:, rows - SUB :, :], "gx", ring("gx", 1))
        xs = [low, lax.ppermute(block[:, :SUB, :], "gx", ring("gx", -1))]
    ys = [lax.ppermute(tail_y, "gy", ring("gy", 1)), lax.ppermute(head_y, "gy", ring("gy", -1))]
    zs = [lax.ppermute(tail_z, "gz", ring("gz", 1)), lax.ppermute(head_z, "gz", ring("gz", -1))]
    return xs, ys + zs


def body(state, diffusivity, rates, inverse, boundary):
    species, nx, ny, lanes = state.shape
    rows = nx * ny
    groups = groups_of(rows)
    assert ny * 2 == SUB and groups % 2 == 0 and lanes == 128
    devices = lax.axis_size("gx") * lax.axis_size("gy") * lax.axis_size("gz")
    entries = float(species * rows * lanes * devices)
    packs = -(-species * groups * 2 // lanes)
    block = shaped(species, rows, lanes)
    faces = [shaped(species, groups // 2 * SUB, lanes)] * 2 + [shaped(packs * SUB, lanes)] * 2
    partial = shaped(devices, lanes)
    flat = pltpu.VMEM((species * SUB, groups * lanes), f32)
    edges = pltpu.VMEM((2, packs * SUB, lanes), f32)

    state = state.reshape(species, rows, lanes)
    inverse = inverse.reshape(species, species, rows, lanes)
    mix, scales, sides = call(
        spread_kernel,
        [
            jax.ShapeDtypeStruct((species * SUB, 3 * species * SUB), jnp.bfloat16),
            shaped(species, SUB, lanes),
            shaped(11, SUB, lanes),
        ],
        [VMEM, SMEM, SMEM],
        (rates, diffusivity, boundary),
        cost=1 << 20,
        name="spread",
    )

    def total(part):
        return lax.all_to_all(part, AXES, 0, 0)

    packed = call(pack_kernel, faces, [VMEM], (state,), cost=1 << 34, name="pack")
    xs, others = exchange(state, *packed)
    n = len(xs)
    rate, weights = call(
        first_local_kernel,
        [block, block],
        [VMEM, SMEM, SMEM],
        (state, diffusivity, boundary),
        cost=1 << 23,
        name="first_local",
    )
    rate0, base, update, part = call(
        functools.partial(first_kernel, n),
        [block, block, block, partial],
        [VMEM] * (n + 11),
        (state, *xs, *others, scales, sides, mix, inverse, rate, weights),
        [flat, flat, edges],
        cost=1 << 23,
        name="first",
    )
    newton = functools.partial(next_kernel, entries)

    def iterate(part, base, update):
        return call(
            newton,
            [block, block, partial],
            [VMEM] * 6,
            (total(part), base, update, weights, mix, inverse),
            [flat, flat],
            cost=8 << 20,
            name="newton",
        )

    for _ in range(NEWTON - 1):
        base, update, part = iterate(part, base, update)
    section = call(
        functools.partial(last_kernel, entries), block, [VMEM] * 3, (total(part), base, update), cost=1 << 19, name="section"
    )
    packed = call(pack_kernel, faces, [VMEM], (section,), cost=1 << 20, name="pack_section")
    xs, others = exchange(section, *packed)
    mixed = call(
        second_local_kernel,
        block,
        [VMEM] + [SMEM, SMEM] + [VMEM] * 3,
        (section, diffusivity, boundary, mix, state, rate0),
        [flat, flat],
        cost=1 << 23,
        name="second_local",
    )
    base, update, part = call(
        functools.partial(second_kernel, n),
        [block, block, partial],
        [VMEM] * (n + 10),
        (mixed, *xs, *others, scales, sides, mix, inverse, weights),
        [flat, flat, edges],
        cost=1 << 23,
        name="second",
    )
    for _ in range(NEWTON - 1):
        base, update, part = iterate(part, base, update)
    out = call(
        functools.partial(last_kernel, entries), block, [VMEM] * 3, (total(part), base, update), cost=1 << 19, name="last"
    )
    return out.reshape(species, nx, ny, lanes)


def solution(mesh):
    in_specs = (P(None, "gx", "gy", "gz"), P(), P(), P(None, None, "gx", "gy", "gz"), P())
    out_specs = P(None, "gx", "gy", "gz")
    return jax.shard_map(body, mesh=mesh, in_specs=in_specs, out_specs=out_specs, check_vma=False)
```

```python
import functools

import jax
import jax.numpy as jnp
from jax import lax
from jax.experimental import pallas as pl
from jax.experimental.pallas import tpu as pltpu
from jax.sharding import PartitionSpec as P

NEWTON = 2
AXES = ("gx", "gy", "gz")
SUB = 8

implicit_gamma = 0.2928932188134524
explicit_delta = -0.7071067811865475
rel_tol = 0.1
abs_tol = 0.05
drift_speed = 0.2

VMEM = pl.BlockSpec(memory_space=pltpu.VMEM)
SMEM = pl.BlockSpec(memory_space=pltpu.SMEM)
f32 = jnp.float32


def iota(dim, lanes):
    return lax.broadcasted_iota(jnp.int32, (SUB, lanes), dim)


def turn(value, shift, axis):
    size = value.shape[axis]
    return pltpu.roll(value, shift % size, axis)


def groups_of(rows):
    return rows // SUB


def pack_faces(load, species, groups, lanes, tail_y, head_y, tail_z, head_z):
    row = iota(0, lanes) % 4
    lane = iota(1, lanes)
    per = lanes // 2
    packs = tail_z.shape[0] // SUB
    tails = [jnp.zeros((SUB, lanes), f32) for _ in range(packs)]
    heads = [jnp.zeros((SUB, lanes), f32) for _ in range(packs)]
    for s in range(species):
        v = [load(s, g) for g in range(groups)]
        for k in range(groups // 2):
            a, b = v[2 * k], v[2 * k + 1]
            tail_y[s, k * SUB : (k + 1) * SUB, :] = jnp.where(row >= 2, a, turn(b, -2, 0))
            head_y[s, k * SUB : (k + 1) * SUB, :] = jnp.where(row < 2, a, turn(b, 2, 0))
        for g in range(groups):
            p, q = divmod(s * groups + g, per)
            here = lane // 2 == q
            tails[p] = jnp.where(here, turn(v[g], 2 * q + 2, 1), tails[p])
            heads[p] = jnp.where(here, turn(v[g], 2 * q, 1), heads[p])
    for p in range(packs):
        tail_z[p * SUB : (p + 1) * SUB, :] = tails[p]
        head_z[p * SUB : (p + 1) * SUB, :] = heads[p]


def wall_flags(kinds):
    out = []
    for i, axis in enumerate(AXES):
        walled = kinds[i] == 0
        here, last = lax.axis_index(axis), lax.axis_size(axis) - 1
        out.append((walled & (here == 0), walled & (here == last)))
    return out


def ghost_terms(low, high, scale, groups, sides):
    near_low, near_high = turn(low, 4, 0), turn(high, 4, 0)
    first = scale * (sides[2] * near_low - sides[0] * low) + sides[4] * near_low
    last = scale * (sides[3] * near_high - sides[1] * high)
    return [first] + [jnp.zeros_like(low)] * (groups - 2) + [last]


def prepare_ends(tail_z, head_z, sides, edges):
    lane = iota(1, tail_z.shape[1])
    even, first = lane % 2 == 0, lane % 4 < 2
    for p in range(tail_z.shape[0] // SUB):
        span = slice(p * SUB, (p + 1) * SUB)
        low, high = tail_z[span, :], head_z[span, :]
        low = (jnp.where(even, 16.0 * turn(low, -1, 1), 0.0) - low) * sides[5]
        high = (jnp.where(even, 0.0, 16.0 * turn(high, 1, 1)) - high) * sides[6]
        high = turn(high, -2, 1)
        edges[0, span, :] = jnp.where(first, low, high)
        edges[1, span, :] = jnp.where(first, high, low)


def row_terms(tail, head, k, sides):
    a01, a0, b23, b3 = sides[7:11]
    span = slice(k * SUB, (k + 1) * SUB)
    t, h = tail[span, :], head[span, :]
    first = a01 * turn(t, -2, 0) + a0 * turn(t, -3, 0) + b23 * turn(h, 2, 0) + b3 * turn(h, 3, 0)
    second = a01 * t + a0 * turn(t, -1, 0) + b23 * h + b3 * turn(h, 1, 0)
    return [first, second]


def end_terms(edges, rows, s, groups, scale):
    lanes = edges.shape[2]
    lane = iota(1, lanes)
    edge = (lane < 2) | (lane >= lanes - 2)
    out = []
    for g in range(groups):
        p, q = divmod(s * groups + g, lanes // 2)
        ends = turn(edges[q % 2, p * SUB : (p + 1) * SUB, :], -2 * q, 1)
        out.append(scale * (rows[g] + jnp.where(edge, ends, 0.0)))
    return out


def transport(load, store, species, groups, lanes, diffusivity, kinds):
    (wall_x0, wall_x1), (wall_y0, wall_y1), (wall_z0, wall_z1) = wall_flags(kinds)
    row = iota(0, lanes) % 4
    lane = iota(1, lanes)
    low_half = iota(0, lanes) < 4
    zero = jnp.zeros((SUB, lanes), f32)

    def along(pos, length, wall0, wall1):
        w0 = jnp.where(wall0, 1.0, 0.0).astype(f32)
        w1 = jnp.where(wall1, 1.0, 0.0).astype(f32)
        at = lambda k: pos == k
        centre = jnp.where(at(0), 16.0 * w0, jnp.where(at(length - 1), 16.0 * w1, 0.0)) - 30.0
        up1 = jnp.where(at(0), 0.0, 16.0) - jnp.where(at(1), w0, 0.0) - jnp.where(at(length - 1), w1, 0.0)
        dn1 = jnp.where(at(length - 1), 0.0, 16.0) - jnp.where(at(0), w0, 0.0) - jnp.where(at(length - 2), w1, 0.0)
        up2 = jnp.where(pos < 2, 0.0, -1.0)
        dn2 = jnp.where(pos >= length - 2, 0.0, -1.0)
        return centre, up1, dn1, up2, dn2

    cy, uy1, dy1, uy2, dy2 = along(row, 4, wall_y0, wall_y1)
    cz, uz1, dz1, uz2, dz2 = along(lane, lanes, wall_z0, wall_z1)
    centre = cy + cz - 30.0

    for s in range(species):
        v = [load(s, g) for g in range(groups)]
        half = [turn(u, 4, 0) for u in v]
        ghost_low = jnp.where(wall_x0, half[0], zero)
        ghost_high = jnp.where(wall_x1, half[-1], zero)
        chain = [ghost_low] + v + [ghost_high]
        halves = [turn(ghost_low, 4, 0)] + half + [turn(ghost_high, 4, 0)]
        scale = diffusivity[s] * (1.0 / 12.0)
        for g in range(groups):
            u = v[g]
            below = jnp.where(low_half, halves[g], halves[g + 1])
            above = jnp.where(low_half, halves[g + 1], halves[g + 2])
            total = centre * u + 16.0 * (below + above) - (chain[g] + chain[g + 2])
            total = total + uy1 * turn(u, 1, 0) + dy1 * turn(u, -1, 0)
            total = total + uy2 * turn(u, 2, 0) + dy2 * turn(u, -2, 0)
            total = total + uz1 * turn(u, 1, 1) + dz1 * turn(u, -1, 1)
            total = total + uz2 * turn(u, 2, 1) + dz2 * turn(u, -2, 1)
            store(s, g, u, scale * total - drift_speed * (u - below))


def stack_parts(parts, size):
    whole = size // 128 * 128
    return jnp.concatenate([p[:whole] for p in parts] + [p[whole:] for p in parts], axis=0)


def spread_kernel(rates, diffusivity, kinds, mix, scales, sides):
    species = rates.shape[0]
    size = species * SUB
    whole = size // 128 * 128
    part = size - whole

    def picks(rows, of):
        hit = of(lax.broadcasted_iota(jnp.int32, (rows, species), 0)) == lax.broadcasted_iota(jnp.int32, (rows, species), 1)
        return jnp.where(hit, 1.0, 0.0).astype(jnp.bfloat16)

    scaled = rates[...] * -implicit_gamma
    high = scaled.astype(jnp.bfloat16)
    low = (scaled - high.astype(f32)).astype(jnp.bfloat16)
    tall = picks(size, lambda i: i >> 3)

    def spread(piece, columns):
        rows = jnp.dot(tall, piece, preferred_element_type=f32).astype(jnp.bfloat16)
        full = lax.dot_general(rows, columns, (((1,), (1,)), ((), ())), preferred_element_type=f32)
        same = lax.broadcasted_iota(jnp.int32, full.shape, 0) & 7 == lax.broadcasted_iota(jnp.int32, full.shape, 1) & 7
        return jnp.where(same, full, 0.0)

    if whole:
        body = picks(whole, lambda i: i >> 3)
        front = spread(high, body).astype(jnp.bfloat16)
        mix[:, :whole] = front
        mix[:, whole : 2 * whole] = front
        mix[:, 2 * whole : 3 * whole] = spread(low, body).astype(jnp.bfloat16)
    if part:
        turns = lambda i: jnp.where(i < part, i, jnp.where(i < 2 * part, i - part, i - 2 * part))
        ends = picks(3 * part, lambda i: (turns(i) + whole) >> 3)
        column = lax.broadcasted_iota(jnp.int32, (size, 3 * part), 1)
        mix[:, 3 * whole :] = jnp.where(column < 2 * part, spread(high, ends), spread(low, ends)).astype(jnp.bfloat16)
    tile = scales.shape[1:]
    for s in range(species):
        scales[s] = jnp.full(tile, diffusivity[s] * (1.0 / 12.0), f32)
    keep = [jnp.where(w, 0.0, 1.0).astype(f32) for pair in wall_flags(kinds) for w in pair]
    keep0, keep1, y0, y1, keep2, keep3 = keep
    low_half = iota(0, tile[1]) < 4
    sides[0] = jnp.full(tile, keep0, f32)
    sides[1] = jnp.full(tile, keep1, f32)
    sides[2] = jnp.where(low_half, 16.0 * keep0, 0.0)
    sides[3] = jnp.where(low_half, 0.0, 16.0 * keep1)
    sides[4] = jnp.where(low_half, drift_speed * keep0, 0.0)
    sides[5] = jnp.full(tile, keep2, f32)
    sides[6] = jnp.full(tile, keep3, f32)
    row = iota(0, tile[1]) % 4
    sides[7] = jnp.where(row < 2, -y0, 0.0)
    sides[8] = jnp.where(row == 0, 16.0 * y0, 0.0)
    sides[9] = jnp.where(row >= 2, -y1, 0.0)
    sides[10] = jnp.where(row == 3, 16.0 * y1, 0.0)


def at(s, g, lanes):
    return slice(s * SUB, (s + 1) * SUB), slice(g * lanes, (g + 1) * lanes)


def chemistry(acts, mix):
    values = acts[...]
    high = values.astype(jnp.bfloat16).astype(f32)
    stack = stack_parts([high, values - high, high], values.shape[0]).astype(jnp.bfloat16)
    return jnp.dot(mix[...], stack, preferred_element_type=f32)


def matvec(inverse, residual, weights, update, partial, species, groups, lanes, block=8):
    def some(first, count, squares):
        out = []
        for h in range(groups):
            span = slice(h * SUB, (h + 1) * SUB)
            acc = [None] * count
            for j in range(species):
                g = residual[at(j, h, lanes)]
                for i in range(count):
                    term = inverse[first + i, j, span, :] * g
                    acc[i] = term if acc[i] is None else acc[i] + term
            total = squares[h]
            for i in range(count):
                update[first + i, span, :] = acc[i]
                scaled = acc[i] * weights[first + i, span, :]
                total = total + scaled * scaled
            out.append(total)
        return tuple(out)

    squares = (jnp.zeros((SUB, lanes), f32),) * groups
    whole = species // block
    squares = lax.fori_loop(0, whole, lambda k, c: some(k * block, block, c), squares)
    if species % block:
        squares = some(whole * block, species % block, squares)
    partial[...] = jnp.broadcast_to(jnp.sum(sum(squares), axis=0, keepdims=True), partial.shape)


def damping(parts, entries):
    total = jnp.sum(parts[...], axis=(0, 1), keepdims=True)
    return 1.0 / jnp.maximum(jnp.sqrt(total * (1.0 / entries)), 1.0)


def pack_kernel(state, tail_y, head_y, tail_z, head_z):
    species, rows, lanes = state.shape
    load = lambda s, g: state[s, g * SUB : (g + 1) * SUB, :]
    pack_faces(load, species, groups_of(rows), lanes, tail_y, head_y, tail_z, head_z)


def face_loads(refs, lanes):
    if len(refs) == 1:
        block = refs[0]
        rows = block.shape[1]
        return (lambda s: block[s, rows - SUB :, :]), (lambda s: block[s, :SUB, :])
    low, high = refs
    return (lambda s: low[s]), (lambda s: high[s])


def first_local_kernel(state, diffusivity, kinds, rate, weights):
    species, rows, lanes = state.shape
    groups = groups_of(rows)

    def store(s, g, u, e):
        span = slice(g * SUB, (g + 1) * SUB)
        rate[s, span, :] = e
        weights[s, span, :] = 1.0 / (rel_tol * jnp.abs(u) + abs_tol)

    load = lambda s, g: state[s, g * SUB : (g + 1) * SUB, :]
    transport(load, store, species, groups, lanes, diffusivity, kinds)


def first_kernel(x_faces, state, *refs):
    xs, refs = refs[:x_faces], refs[x_faces:]
    tail_y, head_y, tail_z, head_z, scales, sides, mix, inverse, rate, weights, rate0, base, update, partial, acts, made, edges = refs
    species, rows, lanes = state.shape
    groups = groups_of(rows)
    low, high = face_loads(xs, lanes)
    sides = [sides[i] for i in range(sides.shape[0])]
    prepare_ends(tail_z, head_z, sides, edges)
    for s in range(species):
        scale = scales[s]
        terms = ghost_terms(low(s), high(s), scale, groups, sides)
        rows_y = [t for k in range(groups // 2) for t in row_terms(tail_y[s], head_y[s], k, sides)]
        terms = [a + b for a, b in zip(terms, end_terms(edges, rows_y, s, groups, scale))]
        for g in range(groups):
            span = slice(g * SUB, (g + 1) * SUB)
            e = rate[s, span, :] + terms[g]
            rate0[s, span, :] = e
            b = state[s, span, :] + implicit_gamma * e
            base[s, span, :] = b
            acts[at(s, g, lanes)] = jnp.tanh(b)
    made[...] = chemistry(acts, mix)
    matvec(inverse, made, weights, update, partial, species, groups, lanes)


def next_kernel(entries, parts, base, update, weights, mix, inverse, guess, second, partial, acts, made):
    species, rows, lanes = base.shape
    groups = groups_of(rows)
    scale = damping(parts, entries)
    for s in range(species):
        for g in range(groups):
            span = slice(g * SUB, (g + 1) * SUB)
            z = base[s, span, :] - update[s, span, :] * scale
            guess[s, span, :] = z
            acts[at(s, g, lanes)] = jnp.tanh(z)
            made[at(s, g, lanes)] = z - base[s, span, :]
    made[...] = made[...] + chemistry(acts, mix)
    matvec(inverse, made, weights, second, partial, species, groups, lanes)


def second_local_kernel(
    section, diffusivity, kinds, mix, state, rate0, mixed, acts, made
):
    species, rows, lanes = state.shape
    groups = groups_of(rows)
    for s in range(species):
        for g in range(groups):
            acts[at(s, g, lanes)] = jnp.tanh(section[s, g * SUB : (g + 1) * SUB, :])
    made[...] = chemistry(acts, mix) * ((1.0 - implicit_gamma) / -implicit_gamma)

    def store(s, g, u, e):
        span = slice(g * SUB, (g + 1) * SUB)
        known = state[s, span, :] + explicit_delta * rate0[s, span, :] + (1.0 - explicit_delta) * e
        mixed[s, span, :] = known + made[at(s, g, lanes)]

    load = lambda s, g: section[s, g * SUB : (g + 1) * SUB, :]
    transport(load, store, species, groups, lanes, diffusivity, kinds)


def second_kernel(x_faces, mixed, *refs):
    xs, refs = refs[:x_faces], refs[x_faces:]
    tail_y, head_y, tail_z, head_z, scales, sides, mix, inverse, weights, base, update, partial, acts, made, edges = refs
    species, rows, lanes = mixed.shape
    groups = groups_of(rows)
    low, high = face_loads(xs, lanes)
    sides = [sides[i] for i in range(sides.shape[0])]
    prepare_ends(tail_z, head_z, sides, edges)
    for s in range(species):
        scale = scales[s]
        terms = ghost_terms(low(s), high(s), scale, groups, sides)
        rows_y = [t for k in range(groups // 2) for t in row_terms(tail_y[s], head_y[s], k, sides)]
        terms = [a + b for a, b in zip(terms, end_terms(edges, rows_y, s, groups, scale))]
        for g in range(groups):
            span = slice(g * SUB, (g + 1) * SUB)
            b = mixed[s, span, :] + (1.0 - explicit_delta) * terms[g]
            base[s, span, :] = b
            acts[at(s, g, lanes)] = jnp.tanh(b)
    made[...] = chemistry(acts, mix)
    matvec(inverse, made, weights, update, partial, species, groups, lanes)


def last_kernel(entries, parts, guess, update, out):
    scale = damping(parts, entries)
    for s in range(guess.shape[0]):
        out[s] = guess[s] - update[s] * scale


def write_kernel(entries, parts, guess, update, out, held, sems):
    scale = damping(parts, entries)
    species, chunks = guess.shape[0], sems.shape[0]
    copies = []
    for c in range(chunks):
        first, stop = c * species // chunks, (c + 1) * species // chunks
        for s in range(first, stop):
            held[s] = guess[s] - update[s] * scale
        span = pl.ds(first, stop - first)
        copies.append(pltpu.make_async_copy(held.at[span], out.at[span], sems.at[c]))
        copies[-1].start()
    for copy in copies:
        copy.wait()


def shaped(*dims):
    return jax.ShapeDtypeStruct(dims, f32)


def call(kernel, outs, specs, args, scratch=(), cost=0, limit=(6 << 20) + 1024, name=None, out_space=pltpu.VMEM):
    return pl.pallas_call(
        kernel,
        out_shape=outs,
        in_specs=specs,
        out_specs=jax.tree.map(lambda _: pl.BlockSpec(memory_space=out_space), outs),
        scratch_shapes=scratch,
        compiler_params=pltpu.CompilerParams(vmem_limit_bytes=limit),
        cost_estimate=pl.CostEstimate(flops=cost, bytes_accessed=cost, transcendentals=0),
        name=name,
    )(*args)


def ring(axis, step):
    count = lax.axis_size(axis)
    return [(i, (i + step) % count) for i in range(count)]


def exchange(block, tail_y, head_y, tail_z, head_z):
    rows = block.shape[1]
    if lax.axis_size("gx") == 2 and rows == 2 * SUB:
        xs = [lax.ppermute(block, "gx", ring("gx", 1))]
    else:
        low = lax.ppermute(block[:, rows - SUB :, :], "gx", ring("gx", 1))
        xs = [low, lax.ppermute(block[:, :SUB, :], "gx", ring("gx", -1))]
    ys = [lax.ppermute(tail_y, "gy", ring("gy", 1)), lax.ppermute(head_y, "gy", ring("gy", -1))]
    zs = [lax.ppermute(tail_z, "gz", ring("gz", 1)), lax.ppermute(head_z, "gz", ring("gz", -1))]
    return xs, ys + zs


def body(state, diffusivity, rates, inverse, boundary):
    species, nx, ny, lanes = state.shape
    rows = nx * ny
    groups = groups_of(rows)
    assert ny * 2 == SUB and groups % 2 == 0 and lanes == 128
    devices = lax.axis_size("gx") * lax.axis_size("gy") * lax.axis_size("gz")
    entries = float(species * rows * lanes * devices)
    packs = -(-species * groups * 2 // lanes)
    block = shaped(species, rows, lanes)
    faces = [shaped(species, groups // 2 * SUB, lanes)] * 2 + [shaped(packs * SUB, lanes)] * 2
    partial = shaped(devices, lanes)
    flat = pltpu.VMEM((species * SUB, groups * lanes), f32)
    edges = pltpu.VMEM((2, packs * SUB, lanes), f32)

    state = state.reshape(species, rows, lanes)
    inverse = inverse.reshape(species, species, rows, lanes)
    mix, scales, sides = call(
        spread_kernel,
        [
            jax.ShapeDtypeStruct((species * SUB, 3 * species * SUB), jnp.bfloat16),
            shaped(species, SUB, lanes),
            shaped(11, SUB, lanes),
        ],
        [VMEM, SMEM, SMEM],
        (rates, diffusivity, boundary),
        cost=1 << 20,
        name="spread",
    )

    def total(part):
        return lax.all_to_all(part, AXES, 0, 0)

    packed = call(pack_kernel, faces, [VMEM], (state,), cost=1 << 34, name="pack")
    xs, others = exchange(state, *packed)
    n = len(xs)
    rate, weights = call(
        first_local_kernel,
        [block, block],
        [VMEM, SMEM, SMEM],
        (state, diffusivity, boundary),
        cost=1 << 23,
        name="first_local",
    )
    rate0, base, update, part = call(
        functools.partial(first_kernel, n),
        [block, block, block, partial],
        [VMEM] * (n + 11),
        (state, *xs, *others, scales, sides, mix, inverse, rate, weights),
        [flat, flat, edges],
        cost=1 << 23,
        name="first",
    )
    newton = functools.partial(next_kernel, entries)

    def iterate(part, base, update):
        return call(
            newton,
            [block, block, partial],
            [VMEM] * 6,
            (total(part), base, update, weights, mix, inverse),
            [flat, flat],
            cost=8 << 20,
            name="newton",
        )

    for _ in range(NEWTON - 1):
        base, update, part = iterate(part, base, update)
    section = call(
        functools.partial(last_kernel, entries), block, [VMEM] * 3, (total(part), base, update), cost=1 << 19, name="section"
    )
    packed = call(pack_kernel, faces, [VMEM], (section,), cost=1 << 20, name="pack_section")
    xs, others = exchange(section, *packed)
    mixed = call(
        second_local_kernel,
        block,
        [VMEM] + [SMEM, SMEM] + [VMEM] * 3,
        (section, diffusivity, boundary, mix, state, rate0),
        [flat, flat],
        cost=1 << 23,
        name="second_local",
    )
    base, update, part = call(
        functools.partial(second_kernel, n),
        [block, block, partial],
        [VMEM] * (n + 10),
        (mixed, *xs, *others, scales, sides, mix, inverse, weights),
        [flat, flat, edges],
        cost=1 << 23,
        name="second",
    )
    for _ in range(NEWTON - 1):
        base, update, part = iterate(part, base, update)
    out = call(
        functools.partial(write_kernel, entries),
        block,
        [VMEM] * 3,
        (total(part), base, update),
        [pltpu.VMEM((species, rows, lanes), f32), pltpu.SemaphoreType.DMA((4,))],
        cost=1 << 19,
        name="last",
        out_space=pl.ANY,
    )
    return out.reshape(species, nx, ny, lanes)


def solution(mesh):
    in_specs = (P(None, "gx", "gy", "gz"), P(), P(), P(None, None, "gx", "gy", "gz"), P())
    out_specs = P(None, "gx", "gy", "gz")
    return jax.shard_map(body, mesh=mesh, in_specs=in_specs, out_specs=out_specs, check_vma=False)
```
